128 devices in a mesh: segment: 2 (over core), gx: 8 (over z_hi, x), gy: 4 (over y), gz: 2 (over z_lo).
Axes of the slice: x: 4, y: 4, z: 4 (z_hi: 2, z_lo: 2; z = z_hi * 2 + z_lo), core: 2. Of those that a mesh axis runs over, the one named last changes fastest.
Arguments:
- features: bfloat16 [2, 16, 32, 128, 256], P(None, None, 'gx', 'gy', 'gz'), may hold values from -6 to 6
- weights: bfloat16 [2, 2, 16, 16, 3, 3, 3], P('segment'), may hold values from -0.4375 to 0.4375
- biases: bfloat16 [2, 2, 16], P('segment'), may hold values from -3 to 3
Outputs:
- section_out: bfloat16 [2, 2, 16, 32, 128, 256], P('segment', None, None, 'gx', 'gy', 'gz')
The draws below stay inside these ranges and needn't reach their ends.
All inputs are finite; a program needn't handle non-finite values.
Results may differ from the reference program's by a relative error of at most 0.0054.
Values may be sent and summed in bfloat16 or wider, within the bound.
A program may use at most 64 MiB of HBM per device.

```python
import jax
import jax.numpy as jnp
from jax import lax

C = 16
MICRO = 2
NX = 32
NY = 128
NZ = 256


def block_scale(key, dims, cuts, least, top_value):
    def one(position, shards_of):
        heights = jax.random.uniform(jax.random.fold_in(jax.random.fold_in(key, 6), position), (shards_of,), jnp.float32, least / len(cuts), top_value / len(cuts))
        return jnp.repeat(jnp.exp(heights), dims[position] // shards_of).reshape((-1,) + (1,) * (len(dims) - position - 1))

    loudness = one(*cuts[0])
    for cut in cuts[1:]:
        loudness = loudness * one(*cut)
    return loudness


def scatter_about(stream_key, shape, scale, limit, cuts=(), held_as=jnp.bfloat16):
    result = scale * jax.random.normal(stream_key, shape, jnp.float32)
    if cuts:
        result = result * block_scale(stream_key, shape, cuts, -0.22, 0.18)
    return jnp.clip(result, -limit, limit).astype(held_as)


def setup_inputs(seed: int = 0) -> dict:
    key_of = jax.random.split(jax.random.key(seed), 4)
    features = scatter_about(key_of[0], (MICRO, C, NX, NY, NZ), 1.0, 6.0, ((2, 8), (3, 4), (4, 2)))
    weights = scatter_about(key_of[1], (2, 2, C, C, 3, 3, 3), (27 * C // 2) ** -0.5, 0.4375, ((0, 2),))
    biases = scatter_about(key_of[2], (2, 2, C), 0.5, 3.0, ((0, 2),))
    return dict(features=features, weights=weights, biases=biases)


def convolve(field, kernel, offset):
    linear = lax.conv_general_dilated(field[None], kernel, (1, 1, 1), ((1, 1), (1, 1), (1, 1)), dimension_numbers=("NCDHW", "OIDHW", "NCDHW"), preferred_element_type=jnp.float32)[0]
    summed = linear + offset.astype(jnp.float32)[:, None, None, None]
    return jnp.where(summed > 0, summed, 0.2 * summed).astype(jnp.bfloat16)


def reference(features, weights, biases):
    first_list = []
    second_list = []
    for batch_index in range(MICRO):
        hidden = features[batch_index]
        hidden = convolve(convolve(hidden, weights[0, 0], biases[0, 0]), weights[0, 1], biases[0, 1])
        first_list.append(hidden)
        hidden = convolve(convolve(hidden, weights[1, 0], biases[1, 0]), weights[1, 1], biases[1, 1])
        second_list.append(hidden)
    return jnp.stack([jnp.stack(first_list), jnp.stack(second_list)])
```

```python
import functools

import jax
import jax.numpy as jnp
from jax import lax
from jax.experimental import pallas as pl
from jax.experimental.pallas import tpu as pltpu
from jax.sharding import PartitionSpec as P

MESH = pl.DeviceIdType.MESH
BF = jnp.bfloat16
F32 = jnp.float32

NXL, NYL, C, L = 4, 32, 16, 128
FX, FY = NXL + 4, NYL + 6
HX, HY = NXL + 2, NYL + 4
KT = 1280


def dots(a, b):
    return jnp.dot(a, b, preferred_element_type=F32)


def leaky(v):
    return jnp.maximum(v, 0.2 * v)


def kernel(
    sizes, feat, wts, bias, out,
    raw, wall, ball, f1, f2, fm, fp, h0, hm, hp, tm, ws, base, brow, wbase, pm, ones,
    eb1, eb2, yb1, yb2, hn, res, stage,
    lsem, wsem, wrs, ssx, rsx, ssy, rsy, ssz, rsz, sso, rso,
):
    ngx, ngy = sizes
    seg, gx = lax.axis_index("segment"), lax.axis_index("gx")
    gy, gz = lax.axis_index("gy"), lax.axis_index("gz")
    has = {
        ("x", 1): gx < ngx - 1, ("x", -1): gx > 0,
        ("y", 1): gy < ngy - 1, ("y", -1): gy > 0,
    }
    here = {"x": gx, "y": gy}

    def to(axis, step):
        return {"g" + axis: here[axis] + step}

    load = pltpu.make_async_copy(feat.at[seg], raw, lsem.at[0])
    load.start()
    wl = pltpu.make_async_copy(wts, wall.at[seg], lsem.at[1])
    wl.start()
    bl = pltpu.make_async_copy(bias, ball.at[seg], lsem.at[2])
    bl.start()

    zrow = jnp.zeros((C, L), BF)

    def clear(ref, x0, x1, y0, y1):
        def body(i, c):
            for y in range(y0, y1):
                ref[i, y] = zrow
            return c
        lax.fori_loop(x0, x1, body, 0)

    for f in (f1, f2):
        clear(f, 0, FX, NYL + 4, FY)
        pl.when(gx == 0)(lambda f=f: clear(f, 0, 2, 0, FY))
        pl.when(gx == ngx - 1)(lambda f=f: clear(f, FX - 2, FX, 0, FY))
        pl.when(gy == 0)(lambda f=f: clear(f, 0, FX, 0, 2))
        pl.when(gy == ngy - 1)(lambda f=f: clear(f, 0, FX, NYL + 2, NYL + 4))
    for e in (eb1, eb2):
        for s in range(2):
            for i in range(FX):
                e[s, i] = zrow
    for e in (yb1, yb2):
        for d in range(2):
            for s in range(2):
                for i in range(NXL):
                    e[d, s, i] = zrow

    bar = pltpu.get_barrier_semaphore()
    for (axis, step), ok in has.items():
        @pl.when(ok)
        def _(axis=axis, step=step):
            pl.semaphore_signal(bar, inc=1, device_id=to(axis, step), device_id_type=MESH)
    pl.semaphore_signal(bar, inc=1, device_id={"gz": 1 - gz}, device_id_type=MESH)
    pl.semaphore_signal(bar, inc=1, device_id={"segment": 1 - seg}, device_id_type=MESH)

    r = lax.broadcasted_iota(jnp.int32, (256, 256), 0)
    c = lax.broadcasted_iota(jnp.int32, (256, 256), 1)
    pm[...] = jnp.where((r // 16 == c % 16) & (r % 16 == c // 16), 1.0, 0.0).astype(BF)
    orow = lax.broadcasted_iota(jnp.int32, (L, L), 0)
    ones[...] = jnp.where(orow < C, 1.0, 0.0).astype(BF)
    load.wait()
    for y in range(NYL // 16):
        for x in range(0, NXL, 2):
            ab = [raw[:, x + k, 16 * y:16 * y + 16, :].reshape(256, L) for k in range(2)]
            t = dots(pm[...], jnp.concatenate(ab, axis=1)).astype(BF)
            for k in range(2):
                f1[x + k + 2, pl.ds(2 + 16 * y, 16)] = t[:, L * k:L * k + L].reshape(16, C, L)

    count = 2 + sum(jnp.where(ok, 1, 0) for ok in has.values())
    pl.semaphore_wait(bar, count)

    def xcopy(q, f, eb, step, k):
        d = 0 if step > 0 else 1
        mv = -NXL * step
        near, far = (FX - 3, FX - 4) if step > 0 else (2, 3)
        lo = FX - 4 if step > 0 else 2
        part = (
            lambda o: f.at[near + o, pl.ds(2, NYL)],
            lambda o: f.at[far + o, pl.ds(2, NYL)],
            lambda o: f.at[pl.ds(lo + o, 2), pl.ds(0, 2)],
            lambda o: f.at[pl.ds(lo + o, 2), pl.ds(NYL + 2, 2)],
            lambda o: eb.at[:, pl.ds(lo + o, 2)],
        )[k]
        return pltpu.make_async_remote_copy(
            part(0), part(mv), ssx.at[q, d, k], rsx.at[q, d, k],
            device_id=to("x", step), device_id_type=MESH)

    def yrows(q, f, step):
        d = 0 if step > 0 else 1
        src, dst = (NYL, 0) if step > 0 else (2, NYL + 2)
        return pltpu.make_async_remote_copy(
            f.at[pl.ds(2, NXL), pl.ds(src, 2)], f.at[pl.ds(2, NXL), pl.ds(dst, 2)],
            ssy.at[q, d, 0], rsy.at[q, d, 0], device_id=to("y", step), device_id_type=MESH)

    def yedges(q, eb, yb, step):
        d = 0 if step > 0 else 1
        return pltpu.make_async_remote_copy(
            eb.at[:, pl.ds(2, NXL)], yb.at[d],
            ssy.at[q, d, 1], rsy.at[q, d, 1], device_id=to("y", step), device_id_type=MESH)

    def zcopy(q, eb):
        return pltpu.make_async_remote_copy(
            eb.at[0, pl.ds(2, NXL)], eb.at[1, pl.ds(2, NXL)], ssz.at[q], rsz.at[q],
            device_id={"gz": 1 - gz}, device_id_type=MESH)

    def ocopy(q):
        return pltpu.make_async_remote_copy(
            stage.at[q], out.at[seg], sso.at[q], rso.at[q],
            device_id={"segment": 1 - seg}, device_id_type=MESH)

    def lcopy(q):
        return pltpu.make_async_copy(stage.at[q], out.at[seg], lsem.at[3 + q])

    def wcopy(k, ref, sec=seg):
        return pltpu.make_async_remote_copy(
            ref.at[sec], ref.at[sec], wsem.at[k], wrs.at[k],
            device_id={"segment": 1 - seg}, device_id_type=MESH)

    lanes = lax.broadcasted_iota(jnp.int32, (C, L), 1)
    edge = jnp.where(gz == 0, L - 1, 0)
    inner = jnp.where(gz == 0, L - 2, 1)

    def pack_edges(f, eb):
        def plane(x, carry):
            def row(y, acc):
                v = f[x, y]
                a = pltpu.roll(v, lax.rem(y + L - edge, L), 1)
                b = pltpu.roll(v, lax.rem(y + 64 + L - inner, L), 1)
                acc = jnp.where(lanes == y, a, acc)
                return jnp.where(lanes == y + 64, b, acc)
            eb[0, x] = lax.fori_loop(2, NYL + 2, row, zrow, unroll=8)
            return carry
        lax.fori_loop(2, NXL + 2, plane, 0)

    def start_exchange(q, f, eb, yb):
        for step in (1, -1):
            @pl.when(has["x", step])
            def _(step=step):
                xcopy(q, f, eb, step, 0).start()
                xcopy(q, f, eb, step, 1).start()
        for step in (1, -1):
            @pl.when(has["y", step])
            def _(step=step):
                yrows(q, f, step).start()
        pack_edges(f, eb)
        zcopy(q, eb).start()

    def middle_exchange(q, f, eb, yb):
        for step in (1, -1):
            @pl.when(has["y", -step])
            def _(step=step):
                yrows(q, f, step).wait_recv()
        for step in (1, -1):
            @pl.when(has["x", step])
            def _(step=step):
                xcopy(q, f, eb, step, 2).start()
                xcopy(q, f, eb, step, 3).start()
        zcopy(q, eb).wait_recv()
        zcopy(q, eb).wait_send()
        for step in (1, -1):
            @pl.when(has["y", step])
            def _(step=step):
                yedges(q, eb, yb, step).start()
        for step in (1, -1):
            @pl.when(has["y", -step])
            def _(step=step):
                yedges(q, eb, yb, step).wait_recv()
            @pl.when(has["y", step])
            def _(step=step):
                yedges(q, eb, yb, step).wait_send()
        low = lanes % 64
        for s in range(2):
            for x in range(NXL):
                v = eb[s, x + 2]
                v = jnp.where(low < 2, pltpu.roll(yb[0, s, x], L - NYL, 1), v)
                v = jnp.where((low >= NYL + 2) & (low < NYL + 4), pltpu.roll(yb[1, s, x], NYL, 1), v)
                eb[s, x + 2] = v
        for step in (1, -1):
            @pl.when(has["x", step])
            def _(step=step):
                xcopy(q, f, eb, step, 4).start()

    def end_exchange(q, f, eb, yb):
        for step in (1, -1):
            @pl.when(has["x", -step])
            def _(step=step):
                for k in range(5):
                    xcopy(q, f, eb, step, k).wait_recv()
            @pl.when(has["x", step])
            def _(step=step):
                for k in range(5):
                    xcopy(q, f, eb, step, k).wait_send()
            @pl.when(has["y", step])
            def _(step=step):
                yrows(q, f, step).wait_send()

    def make_weights(sec):
        for lay in range(2):
            base[...] = jnp.zeros_like(base)
            for dz in range(3):
                for dx in range(3):
                    for dy in range(3):
                        p = 16 * (dx * 6 + dy)
                        base[dz, :, p:p + 16] = wall[sec, lay, dx * 9 + dy * 3 + dz].astype(F32)
            brow[0:1, 0:C] = ball[sec, lay:lay + 1, :].astype(F32)
            for xq in range(2):
                for yq in range(4):
                    rows = slice(16 * (4 * xq + yq), 16 * (4 * xq + yq) + 16)
                    for dz in range(3):
                        v = base[dz]
                        if 6 * xq + yq:
                            v = pltpu.roll(v, 16 * (6 * xq + yq), 1)
                        tm[2 * sec + lay, rows, 384 * dz:384 * dz + 384] = v.astype(BF)
            br = jnp.broadcast_to(brow[0:1, :], (L, L))
            rr = lax.broadcasted_iota(jnp.int32, (L, L), 0)
            cc = lax.broadcasted_iota(jnp.int32, (L, L), 1)
            diag = jnp.where(rr % 16 == cc, br, 0.0).astype(BF)
            tm[2 * sec + lay, :, 1152:1280] = diag
            if lay == 0:
                wbase[...] = jnp.zeros_like(wbase)
                for dy in range(3):
                    for dx in range(3):
                        for col in range(3):
                            p = 16 * (dx * 3 + col)
                            dz = jnp.where(gz == 0, col, 2 - col)
                            wbase[16 * dy:16 * dy + 16, p:p + 16] = wall[
                                sec, 0, dx * 9 + dy * 3 + dz].astype(F32)
                wbase[16:32, 144:160] = diag[0:16, 0:16].astype(F32)
                ws[sec] = wbase[...].astype(BF)

    def shift_rows(f, eb):
        def plane(x, carry):
            n = eb[1, x]
            def row(y, cc):
                v = f[x, y]
                h = pltpu.roll(n, lax.rem(edge + L - y, L), 1)
                h = jnp.where(lanes == edge, h, zrow)
                fm[x, y] = jnp.where(lanes == 0, h, pltpu.roll(v, 1, 1))
                fp[x, y] = jnp.where(lanes == L - 1, h, pltpu.roll(v, L - 1, 1))
                return cc
            lax.fori_loop(0, NYL + 4, row, 0, unroll=6)
            for y in range(NYL + 4, FY):
                fm[x, y] = zrow
                fp[x, y] = zrow
            return carry
        lax.fori_loop(0, FX, plane, 0)

    def strips(sec, eb):
        one = ones[0:C, :]
        tail = jnp.zeros((256 - 160, L), BF)
        lane = lax.broadcasted_iota(jnp.int32, (C, L), 1)
        for j in range(HX):
            rows = []
            for dx in range(3):
                rows += [eb[0, j + dx], eb[1, j + dx], pltpu.roll(eb[1, j + dx], 64, 1)]
            m = dots(ws[sec], jnp.concatenate(rows + [one, tail], axis=0))
            v = pltpu.roll(m[0:16], 1, 1) + m[16:32] + pltpu.roll(m[32:48], L - 1, 1)
            v = leaky(v)
            bad = (lane == 1) & (gy == 0) | (lane == NYL + 2) & (gy == ngy - 1)
            if j == 0:
                bad = bad | (gx == 0)
            if j == HX - 1:
                bad = bad | (gx == ngx - 1)
            hn[j] = jnp.where(bad, 0.0, v).astype(BF)

    def boxes(lay, fields, pairs):
        cols = []
        for x0, y0 in pairs:
            rows = []
            for f in fields:
                for xr in range(4):
                    rows.append(f[x0 + xr, pl.ds(y0, 6)].reshape(96, L))
            cols.append(jnp.concatenate(rows + [ones[...]], axis=0))
        return dots(tm[lay], jnp.concatenate(cols, axis=1))

    def layer_a(sec, f):
        def body(yt, carry):
            y0 = 4 * yt
            pairs = [(0, y0), (2, y0), (4, y0)]
            v = leaky(boxes(2 * sec, (fm, f, fp), pairs)).astype(BF)
            for k, (x0, _) in enumerate(pairs):
                b = v[:, L * k:L * k + L].reshape(2, 4, C, L)
                for xq in range(2):
                    n = hn[x0 + xq]
                    for yq in range(4):
                        t = b[xq, yq]
                        h = pltpu.roll(n, lax.rem(edge + 2 * L - 1 - y0 - yq, L), 1)
                        h = jnp.where(lanes == edge, h, zrow)
                        h0[x0 + xq, y0 + yq] = t
                        hm[x0 + xq, y0 + yq] = jnp.where(lanes == 0, h, pltpu.roll(t, 1, 1))
                        hp[x0 + xq, y0 + yq] = jnp.where(lanes == L - 1, h, pltpu.roll(t, L - 1, 1))
            return carry
        lax.fori_loop(0, HY // 4, body, 0)
        for ref in (h0, hm, hp):
            pl.when(gx == 0)(lambda ref=ref: clear(ref, 0, 1, 0, HY))
            pl.when(gx == ngx - 1)(lambda ref=ref: clear(ref, HX - 1, HX, 0, HY))
            pl.when(gy == 0)(lambda ref=ref: clear(ref, 0, HX, 0, 1))
            pl.when(gy == ngy - 1)(lambda ref=ref: clear(ref, 0, HX, NYL + 1, NYL + 2))

    def layer_b(sec, g, gx0, gy0):
        def body(yt, carry):
            y0 = 4 * yt
            pairs = [(0, y0), (2, y0)]
            v = leaky(boxes(2 * sec + 1, (hm, h0, hp), pairs)).astype(BF)
            for k, (x0, _) in enumerate(pairs):
                b = v[:, L * k:L * k + L].reshape(2, 4, C, L)
                for xq in range(2):
                    g[gx0 + x0 + xq, pl.ds(gy0 + y0, 4)] = b[xq]
            return carry
        lax.fori_loop(0, NYL // 4, body, 0)

    def to_stage(q, g, gx0, gy0):
        for y in range(NYL // 16):
            for x in range(0, NXL, 2):
                ab = [g[gx0 + x + k, pl.ds(gy0 + 16 * y, 16)].reshape(256, L) for k in range(2)]
                t = dots(pm[...], jnp.concatenate(ab, axis=1)).astype(BF)
                for k in range(2):
                    stage[q, :, x + k, 16 * y:16 * y + 16, :] = t[:, L * k:L * k + L].reshape(C, 16, L)

    def send_out(q):
        @pl.when(seg == q)
        def _():
            lcopy(q).start()
        @pl.when(seg != q)
        def _():
            ocopy(q).start()

    start_exchange(0, f1, eb1, yb1)
    wl.wait()
    bl.wait()
    wcopy(0, wall).start()
    wcopy(1, ball).start()
    middle_exchange(0, f1, eb1, yb1)
    brow[...] = jnp.zeros_like(brow)
    wcopy(0, wall, 1 - seg).wait_recv()
    wcopy(1, ball, 1 - seg).wait_recv()
    wcopy(0, wall).wait_send()
    wcopy(1, ball).wait_send()
    for sec in range(2):
        make_weights(sec)
    end_exchange(0, f1, eb1, yb1)

    shift_rows(f1, eb1)
    strips(0, eb1)
    layer_a(0, f1)
    layer_b(0, f2, 2, 2)

    start_exchange(1, f2, eb2, yb2)
    to_stage(0, f2, 2, 2)
    send_out(0)
    middle_exchange(1, f2, eb2, yb2)
    end_exchange(1, f2, eb2, yb2)

    shift_rows(f2, eb2)
    strips(1, eb2)
    layer_a(1, f2)
    layer_b(1, res, 0, 0)
    to_stage(1, res, 0, 0)
    send_out(1)

    for q in range(2):
        @pl.when(seg == q)
        def _(q=q):
            lcopy(q).wait()
            pltpu.make_async_remote_copy(
                stage.at[q], out.at[1 - seg], sso.at[q], rso.at[q],
                device_id={"segment": 1 - seg}, device_id_type=MESH).wait_recv()
        @pl.when(seg != q)
        def _(q=q):
            ocopy(q).wait_send()


def shards(sizes, features, weights, biases):
    w = weights[0].transpose(0, 3, 4, 5, 1, 2).reshape(2, 27, C, C)
    any_space = pl.BlockSpec(memory_space=pl.ANY)
    dma = pltpu.SemaphoreType.DMA
    out = pl.pallas_call(
        functools.partial(kernel, sizes),
        name="sections",
        out_shape=jax.ShapeDtypeStruct((2, C, NXL, NYL, L), BF),
        in_specs=[any_space] * 3,
        out_specs=any_space,
        scratch_shapes=[
            pltpu.VMEM((C, NXL, NYL, L), BF),
            pltpu.VMEM((2, 2, 27, C, C), BF),
            pltpu.VMEM((2, 2, C), BF),
            pltpu.VMEM((FX, FY, C, L), BF),
            pltpu.VMEM((FX, FY, C, L), BF),
            pltpu.VMEM((FX, FY, C, L), BF),
            pltpu.VMEM((FX, FY, C, L), BF),
            pltpu.VMEM((HX, HY, C, L), BF),
            pltpu.VMEM((HX, HY, C, L), BF),
            pltpu.VMEM((HX, HY, C, L), BF),
            pltpu.VMEM((4, L, KT), BF),
            pltpu.VMEM((2, 48, 256), BF),
            pltpu.VMEM((3, C, 384), F32),
            pltpu.VMEM((8, L), F32),
            pltpu.VMEM((48, 256), F32),
            pltpu.VMEM((256, 256), BF),
            pltpu.VMEM((L, L), BF),
            pltpu.VMEM((2, FX, C, L), BF),
            pltpu.VMEM((2, FX, C, L), BF),
            pltpu.VMEM((2, 2, NXL, C, L), BF),
            pltpu.VMEM((2, 2, NXL, C, L), BF),
            pltpu.VMEM((HX, C, L), BF),
            pltpu.VMEM((NXL, NYL, C, L), BF),
            pltpu.VMEM((2, C, NXL, NYL, L), BF),
            dma((5,)), dma((2,)), dma((2,)),
            dma((2, 2, 5)), dma((2, 2, 5)),
            dma((2, 2, 2)), dma((2, 2, 2)),
            dma((2,)), dma((2,)), dma((2,)), dma((2,)),
        ],
        compiler_params=pltpu.CompilerParams(
            collective_id=0, has_side_effects=True, vmem_limit_bytes=60 << 20),
    )(features, w, biases[0])
    return out[None]


def solution(mesh):
    placed = (
        P(None, None, "gx", "gy", "gz"),
        P("segment", None, None, None, None, None, None),
        P("segment", None, None),
    )
    sizes = (mesh.shape["gx"], mesh.shape["gy"])
    return jax.shard_map(
        functools.partial(shards, sizes),
        mesh=mesh,
        in_specs=placed,
        out_specs=P("segment", None, None, "gx", "gy", "gz"),
        check_vma=False,
    )
```

```python
import functools

import jax
import jax.numpy as jnp
from jax import lax
from jax.experimental import pallas as pl
from jax.experimental.pallas import tpu as pltpu
from jax.sharding import PartitionSpec as P

MESH = pl.DeviceIdType.MESH
BF = jnp.bfloat16
F32 = jnp.float32

NXL, NYL, C, L = 4, 32, 16, 128
FX, FY = NXL + 4, NYL + 6
HX, HY = NXL + 2, NYL + 4
KT = 1280


def dots(a, b):
    return jnp.dot(a, b, preferred_element_type=F32)


def iota(shape, dim):
    return lax.broadcasted_iota(jnp.int32, shape, dim)


def one_hot(hit):
    return jnp.where(hit, 1.0, 0.0).astype(BF)


def leaky(v):
    return jnp.maximum(v, 0.2 * v)


def kernel(
    sizes, feat, wts, bias, out,
    raw, wall, ball, f1, f2, fm, fp, h0, hm, hp, tm, ws, base, brow, wbase, pm, ones, sh, sy, xe,
    eb1, eb2, yb1, yb2, hn, res, stage,
    lsem, wsem, wrs, ssx, rsx, ssy, rsy, ssz, rsz, sso, rso,
):
    ngx, ngy = sizes
    seg, gx = lax.axis_index("segment"), lax.axis_index("gx")
    gy, gz = lax.axis_index("gy"), lax.axis_index("gz")
    has = {
        ("x", 1): gx < ngx - 1, ("x", -1): gx > 0,
        ("y", 1): gy < ngy - 1, ("y", -1): gy > 0,
    }
    here = {"x": gx, "y": gy}

    def to(axis, step):
        return {"g" + axis: here[axis] + step}

    lanes = iota((C, L), 1)
    edge = jnp.where(gz == 0, L - 1, 0)
    inner = jnp.where(gz == 0, L - 2, 1)

    load = pltpu.make_async_copy(feat.at[seg], raw, lsem.at[0])
    load.start()
    wl = pltpu.make_async_copy(wts, wall.at[seg], lsem.at[1])
    wl.start()
    bl = pltpu.make_async_copy(bias, ball.at[seg], lsem.at[2])
    bl.start()

    zrow = jnp.zeros((C, L), BF)

    def clear(ref, x0, x1, y0, y1):
        def body(i, c):
            for y in range(y0, y1):
                ref[i, y] = zrow
            return c
        lax.fori_loop(x0, x1, body, 0)

    for f in (f1, f2):
        clear(f, 0, FX, NYL + 4, FY)
        pl.when(gx == 0)(lambda f=f: clear(f, 0, 2, 0, FY))
        pl.when(gx == ngx - 1)(lambda f=f: clear(f, FX - 2, FX, 0, FY))
        pl.when(gy == 0)(lambda f=f: clear(f, 0, FX, 0, 2))
        pl.when(gy == ngy - 1)(lambda f=f: clear(f, 0, FX, NYL + 2, NYL + 4))
    for e in (eb1, eb2):
        for s in range(2):
            for i in range(FX):
                e[s, i] = zrow
    for e in (yb1, yb2):
        for d in range(2):
            for s in range(2):
                for i in range(NXL):
                    e[d, s, i] = zrow

    bar = pltpu.get_barrier_semaphore()
    for (axis, step), ok in has.items():
        @pl.when(ok)
        def _(axis=axis, step=step):
            pl.semaphore_signal(bar, inc=1, device_id=to(axis, step), device_id_type=MESH)
    pl.semaphore_signal(bar, inc=1, device_id={"gz": 1 - gz}, device_id_type=MESH)
    pl.semaphore_signal(bar, inc=1, device_id={"segment": 1 - seg}, device_id_type=MESH)

    r = lax.broadcasted_iota(jnp.int32, (256, 256), 0)
    c = lax.broadcasted_iota(jnp.int32, (256, 256), 1)
    pm[...] = jnp.where((r // 16 == c % 16) & (r % 16 == c // 16), 1.0, 0.0).astype(BF)
    orow = lax.broadcasted_iota(jnp.int32, (L, L), 0)
    ones[...] = jnp.where(orow < C, 1.0, 0.0).astype(BF)
    rl, cl = iota((L, 2 * L), 0), iota((L, 2 * L), 1)
    sh[...] = one_hot((cl < L) & (rl == cl - 1) | (cl >= L) & (rl == cl - L + 1))
    target = jnp.where(gz == 0, 2 * L - 1, 0)
    def table_s(i, carry):
        sy[i] = one_hot((rl == i) & (cl == target))
        return carry
    re, ce = iota((L, L), 0), iota((L, L), 1)
    def table_e(y, carry):
        hit = (re == edge) & (ce == y + 2) | (re == inner) & (ce == y + 66)
        xe[pl.ds(pl.multiple_of(L * y, L), L), :] = one_hot(hit)
        return carry
    lax.fori_loop(0, NYL, table_e, 0)
    load.wait()
    for y in range(NYL // 16):
        for x in range(0, NXL, 2):
            ab = [raw[:, x + k, 16 * y:16 * y + 16, :].reshape(256, L) for k in range(2)]
            t = dots(pm[...], jnp.concatenate(ab, axis=1)).astype(BF)
            for k in range(2):
                f1[x + k + 2, pl.ds(2 + 16 * y, 16)] = t[:, L * k:L * k + L].reshape(16, C, L)

    count = 2 + sum(jnp.where(ok, 1, 0) for ok in has.values())
    pl.semaphore_wait(bar, count)

    def xcopy(q, f, eb, step, k):
        d = 0 if step > 0 else 1
        mv = -NXL * step
        near, far = (FX - 3, FX - 4) if step > 0 else (2, 3)
        lo = FX - 4 if step > 0 else 2
        part = (
            lambda o: f.at[near + o, pl.ds(2, NYL)],
            lambda o: f.at[far + o, pl.ds(2, NYL)],
            lambda o: f.at[pl.ds(lo + o, 2), pl.ds(0, 2)],
            lambda o: f.at[pl.ds(lo + o, 2), pl.ds(NYL + 2, 2)],
            lambda o: eb.at[:, pl.ds(lo + o, 2)],
        )[k]
        return pltpu.make_async_remote_copy(
            part(0), part(mv), ssx.at[q, d, k], rsx.at[q, d, k],
            device_id=to("x", step), device_id_type=MESH)

    def yrows(q, f, step):
        d = 0 if step > 0 else 1
        src, dst = (NYL, 0) if step > 0 else (2, NYL + 2)
        return pltpu.make_async_remote_copy(
            f.at[pl.ds(2, NXL), pl.ds(src, 2)], f.at[pl.ds(2, NXL), pl.ds(dst, 2)],
            ssy.at[q, d, 0], rsy.at[q, d, 0], device_id=to("y", step), device_id_type=MESH)

    def yedges(q, eb, yb, step):
        d = 0 if step > 0 else 1
        return pltpu.make_async_remote_copy(
            eb.at[:, pl.ds(2, NXL)], yb.at[d],
            ssy.at[q, d, 1], rsy.at[q, d, 1], device_id=to("y", step), device_id_type=MESH)

    def zcopy(q, eb):
        return pltpu.make_async_remote_copy(
            eb.at[0, pl.ds(2, NXL)], eb.at[1, pl.ds(2, NXL)], ssz.at[q], rsz.at[q],
            device_id={"gz": 1 - gz}, device_id_type=MESH)

    def ocopy(q):
        return pltpu.make_async_remote_copy(
            stage.at[q], out.at[seg], sso.at[q], rso.at[q],
            device_id={"segment": 1 - seg}, device_id_type=MESH)

    def lcopy(q):
        return pltpu.make_async_copy(stage.at[q], out.at[seg], lsem.at[3 + q])

    def wcopy(k, ref, sec=seg):
        return pltpu.make_async_remote_copy(
            ref.at[sec], ref.at[sec], wsem.at[k], wrs.at[k],
            device_id={"segment": 1 - seg}, device_id_type=MESH)


    def pack_edges(f, eb):
        acc = None
        for y in range(0, NYL, 2):
            lhs = [f[pl.ds(2, NXL), 2 + y + k].reshape(NXL * C, L) for k in range(2)]
            t = dots(jnp.concatenate(lhs, axis=1), xe[pl.ds(L * y, 2 * L), :])
            acc = t if acc is None else acc + t
        eb[0, pl.ds(2, NXL)] = acc.astype(BF).reshape(NXL, C, L)

    def start_exchange(q, f, eb, yb):
        for step in (1, -1):
            @pl.when(has["x", step])
            def _(step=step):
                xcopy(q, f, eb, step, 0).start()
                xcopy(q, f, eb, step, 1).start()
        for step in (1, -1):
            @pl.when(has["y", step])
            def _(step=step):
                yrows(q, f, step).start()
        pack_edges(f, eb)
        zcopy(q, eb).start()

    def middle_exchange(q, f, eb, yb):
        for step in (1, -1):
            @pl.when(has["y", -step])
            def _(step=step):
                yrows(q, f, step).wait_recv()
        for step in (1, -1):
            @pl.when(has["x", step])
            def _(step=step):
                xcopy(q, f, eb, step, 2).start()
                xcopy(q, f, eb, step, 3).start()
        zcopy(q, eb).wait_recv()
        zcopy(q, eb).wait_send()
        for step in (1, -1):
            @pl.when(has["y", step])
            def _(step=step):
                yedges(q, eb, yb, step).start()
        for step in (1, -1):
            @pl.when(has["y", -step])
            def _(step=step):
                yedges(q, eb, yb, step).wait_recv()
            @pl.when(has["y", step])
            def _(step=step):
                yedges(q, eb, yb, step).wait_send()
        low = lanes % 64
        for s in range(2):
            for x in range(NXL):
                v = eb[s, x + 2]
                v = jnp.where(low < 2, pltpu.roll(yb[0, s, x], L - NYL, 1), v)
                v = jnp.where((low >= NYL + 2) & (low < NYL + 4), pltpu.roll(yb[1, s, x], NYL, 1), v)
                eb[s, x + 2] = v
        for step in (1, -1):
            @pl.when(has["x", step])
            def _(step=step):
                xcopy(q, f, eb, step, 4).start()

    def end_exchange(q, f, eb, yb):
        for step in (1, -1):
            @pl.when(has["x", -step])
            def _(step=step):
                for k in range(5):
                    xcopy(q, f, eb, step, k).wait_recv()
            @pl.when(has["x", step])
            def _(step=step):
                for k in range(5):
                    xcopy(q, f, eb, step, k).wait_send()
            @pl.when(has["y", step])
            def _(step=step):
                yrows(q, f, step).wait_send()

    def make_weights(sec):
        for lay in range(2):
            base[...] = jnp.zeros_like(base)
            for dz in range(3):
                for dx in range(3):
                    for dy in range(3):
                        p = 16 * (dx * 6 + dy)
                        base[dz, :, p:p + 16] = wall[sec, lay, dx * 9 + dy * 3 + dz].astype(F32)
            brow[0:1, 0:C] = ball[sec, lay:lay + 1, :].astype(F32)
            for xq in range(2):
                for yq in range(4):
                    rows = slice(16 * (4 * xq + yq), 16 * (4 * xq + yq) + 16)
                    for dz in range(3):
                        v = base[dz]
                        if 6 * xq + yq:
                            v = pltpu.roll(v, 16 * (6 * xq + yq), 1)
                        tm[2 * sec + lay, rows, 384 * dz:384 * dz + 384] = v.astype(BF)
            br = jnp.broadcast_to(brow[0:1, :], (L, L))
            rr = lax.broadcasted_iota(jnp.int32, (L, L), 0)
            cc = lax.broadcasted_iota(jnp.int32, (L, L), 1)
            diag = jnp.where(rr % 16 == cc, br, 0.0).astype(BF)
            tm[2 * sec + lay, :, 1152:1280] = diag
            if lay == 0:
                wbase[...] = jnp.zeros_like(wbase)
                for dy in range(3):
                    for dx in range(3):
                        for col in range(3):
                            p = 16 * (dx * 3 + col)
                            dz = jnp.where(gz == 0, col, 2 - col)
                            wbase[16 * dy:16 * dy + 16, p:p + 16] = wall[
                                sec, 0, dx * 9 + dy * 3 + dz].astype(F32)
                wbase[16:32, 144:160] = diag[0:16, 0:16].astype(F32)
                ws[sec] = wbase[...].astype(BF)

    def shift(src, edges, n, first, dm, dp):
        def body(i, carry):
            e = edges.reshape(n * C, L)
            for k in range(4):
                y = 4 * i + k
                lhs = jnp.concatenate([src[:, y].reshape(n * C, L), e], axis=1)
                rhs = jnp.concatenate([sh[...], sy[first + y]], axis=0)
                t = dots(lhs, rhs).astype(BF)
                dm[:, y] = t[:, :L].reshape(n, C, L)
                dp[:, y] = t[:, L:].reshape(n, C, L)
            return carry
        lax.fori_loop(0, HY // 4, body, 0)

    def strips(sec, eb):
        one = ones[0:C, :]
        tail = jnp.zeros((256 - 160, L), BF)
        lane = lax.broadcasted_iota(jnp.int32, (C, L), 1)
        for j in range(HX):
            rows = []
            for dx in range(3):
                rows += [eb[0, j + dx], eb[1, j + dx], pltpu.roll(eb[1, j + dx], 64, 1)]
            m = dots(ws[sec], jnp.concatenate(rows + [one, tail], axis=0))
            v = pltpu.roll(m[0:16], 1, 1) + m[16:32] + pltpu.roll(m[32:48], L - 1, 1)
            v = leaky(v)
            bad = (lane == 1) & (gy == 0) | (lane == NYL + 2) & (gy == ngy - 1)
            if j == 0:
                bad = bad | (gx == 0)
            if j == HX - 1:
                bad = bad | (gx == ngx - 1)
            hn[j] = jnp.where(bad, 0.0, v).astype(BF)

    def boxes(lay, fields, pairs):
        acc = None
        for k in range(5):
            cols = []
            for x0, y0 in pairs:
                rows = []
                for p in range(16 * k, min(16 * k + 16, 72)):
                    g, yr = divmod(p, 6)
                    rows.append(fields[g // 4][x0 + g % 4, y0 + yr])
                if k == 4:
                    rows.append(ones[...])
                cols.append(jnp.concatenate(rows, axis=0))
            t = dots(tm[lay, :, 256 * k:256 * k + 256], jnp.concatenate(cols, axis=1))
            acc = t if acc is None else acc + t
        return leaky(acc).astype(BF)

    def layer(lay, fields, todo, n, dst, ox, oy):
        def body(i, carry):
            pairs = [todo(4 * i + k) for k in range(4)]
            for h in range(2):
                v = boxes(lay, fields, pairs[2 * h:2 * h + 2])
                for k in range(2):
                    x0, y0 = pairs[2 * h + k]
                    b = v[:, L * k:L * k + L].reshape(2, 4, C, L)
                    for xq in range(2):
                        dst[ox + x0 + xq, pl.ds(oy + y0, 4)] = b[xq]
            return carry
        lax.fori_loop(0, (n + 3) // 4, body, 0)

    def layer_a(sec, f):
        def todo(j):
            j = jnp.minimum(j, 26)
            return 2 * lax.rem(j, 3), 4 * lax.div(j, 3)
        layer(2 * sec, (fm, f, fp), todo, 27, h0, 0, 0)
        pl.when(gx == 0)(lambda: clear(h0, 0, 1, 0, HY))
        pl.when(gx == ngx - 1)(lambda: clear(h0, HX - 1, HX, 0, HY))
        pl.when(gy == 0)(lambda: clear(h0, 0, HX, 0, 1))
        pl.when(gy == ngy - 1)(lambda: clear(h0, 0, HX, NYL + 1, NYL + 2))

    def layer_b(sec, g, gx0, gy0):
        layer(2 * sec + 1, (hm, h0, hp), lambda j: (2 * lax.rem(j, 2), 4 * lax.div(j, 2)), 16, g, gx0, gy0)

    def to_stage(q, g, gx0, gy0):
        for y in range(NYL // 16):
            for x in range(0, NXL, 2):
                ab = [g[gx0 + x + k, pl.ds(gy0 + 16 * y, 16)].reshape(256, L) for k in range(2)]
                t = dots(pm[...], jnp.concatenate(ab, axis=1)).astype(BF)
                for k in range(2):
                    stage[q, :, x + k, 16 * y:16 * y + 16, :] = t[:, L * k:L * k + L].reshape(C, 16, L)

    def send_out(q):
        @pl.when(seg == q)
        def _():
            lcopy(q).start()
        @pl.when(seg != q)
        def _():
            ocopy(q).start()

    start_exchange(0, f1, eb1, yb1)
    wl.wait()
    bl.wait()
    wcopy(0, wall).start()
    wcopy(1, ball).start()
    middle_exchange(0, f1, eb1, yb1)
    brow[...] = jnp.zeros_like(brow)
    wcopy(0, wall, 1 - seg).wait_recv()
    wcopy(1, ball, 1 - seg).wait_recv()
    wcopy(0, wall).wait_send()
    wcopy(1, ball).wait_send()
    lax.fori_loop(0, HY + 1, table_s, 0)
    for f in (fm, fp):
        clear(f, 0, FX, NYL + 4, FY)
    for sec in range(2):
        make_weights(sec)
    end_exchange(0, f1, eb1, yb1)

    shift(f1, eb1[1], FX, 0, fm, fp)
    strips(0, eb1)
    layer_a(0, f1)
    shift(h0, hn[...], HX, 1, hm, hp)
    layer_b(0, f2, 2, 2)

    start_exchange(1, f2, eb2, yb2)
    to_stage(0, f2, 2, 2)
    send_out(0)
    middle_exchange(1, f2, eb2, yb2)
    end_exchange(1, f2, eb2, yb2)

    shift(f2, eb2[1], FX, 0, fm, fp)
    strips(1, eb2)
    layer_a(1, f2)
    shift(h0, hn[...], HX, 1, hm, hp)
    layer_b(1, res, 0, 0)
    to_stage(1, res, 0, 0)
    send_out(1)

    for q in range(2):
        @pl.when(seg == q)
        def _(q=q):
            lcopy(q).wait()
            pltpu.make_async_remote_copy(
                stage.at[q], out.at[1 - seg], sso.at[q], rso.at[q],
                device_id={"segment": 1 - seg}, device_id_type=MESH).wait_recv()
        @pl.when(seg != q)
        def _(q=q):
            ocopy(q).wait_send()


def shards(sizes, features, weights, biases):
    w = weights[0].transpose(0, 3, 4, 5, 1, 2).reshape(2, 27, C, C)
    any_space = pl.BlockSpec(memory_space=pl.ANY)
    dma = pltpu.SemaphoreType.DMA
    out = pl.pallas_call(
        functools.partial(kernel, sizes),
        name="sections",
        out_shape=jax.ShapeDtypeStruct((2, C, NXL, NYL, L), BF),
        in_specs=[any_space] * 3,
        out_specs=any_space,
        scratch_shapes=[
            pltpu.VMEM((C, NXL, NYL, L), BF),
            pltpu.VMEM((2, 2, 27, C, C), BF),
            pltpu.VMEM((2, 2, C), BF),
            pltpu.VMEM((FX, FY, C, L), BF),
            pltpu.VMEM((FX, FY, C, L), BF),
            pltpu.VMEM((FX, FY, C, L), BF),
            pltpu.VMEM((FX, FY, C, L), BF),
            pltpu.VMEM((HX, HY, C, L), BF),
            pltpu.VMEM((HX, HY, C, L), BF),
            pltpu.VMEM((HX, HY, C, L), BF),
            pltpu.VMEM((4, L, KT), BF),
            pltpu.VMEM((2, 48, 256), BF),
            pltpu.VMEM((3, C, 384), F32),
            pltpu.VMEM((8, L), F32),
            pltpu.VMEM((48, 256), F32),
            pltpu.VMEM((256, 256), BF),
            pltpu.VMEM((L, L), BF),
            pltpu.VMEM((L, 2 * L), BF),
            pltpu.VMEM((HY + 1, L, 2 * L), BF),
            pltpu.VMEM((NYL * L, L), BF),
            pltpu.VMEM((2, FX, C, L), BF),
            pltpu.VMEM((2, FX, C, L), BF),
            pltpu.VMEM((2, 2, NXL, C, L), BF),
            pltpu.VMEM((2, 2, NXL, C, L), BF),
            pltpu.VMEM((HX, C, L), BF),
            pltpu.VMEM((NXL, NYL, C, L), BF),
            pltpu.VMEM((2, C, NXL, NYL, L), BF),
            dma((5,)), dma((2,)), dma((2,)),
            dma((2, 2, 5)), dma((2, 2, 5)),
            dma((2, 2, 2)), dma((2, 2, 2)),
            dma((2,)), dma((2,)), dma((2,)), dma((2,)),
        ],
        compiler_params=pltpu.CompilerParams(
            collective_id=0, has_side_effects=True, vmem_limit_bytes=60 << 20),
    )(features, w, biases[0])
    return out[None]


def solution(mesh):
    placed = (
        P(None, None, "gx", "gy", "gz"),
        P("segment", None, None, None, None, None, None),
        P("segment", None, None),
    )
    sizes = (mesh.shape["gx"], mesh.shape["gy"])
    return jax.shard_map(
        functools.partial(shards, sizes),
        mesh=mesh,
        in_specs=placed,
        out_specs=P("segment", None, None, "gx", "gy", "gz"),
        check_vma=False,
    )
```

```python
import functools

import jax
import jax.numpy as jnp
from jax import lax
from jax.experimental import pallas as pl
from jax.experimental.pallas import tpu as pltpu
from jax.sharding import PartitionSpec as P

MESH = pl.DeviceIdType.MESH
BF = jnp.bfloat16
F32 = jnp.float32

NXL, NYL, C, L = 4, 32, 16, 128
FX, FY = NXL + 4, NYL + 6
HX, HY = NXL + 2, NYL + 4
KT = 1280


def dots(a, b):
    return jnp.dot(a, b, preferred_element_type=F32)


def iota(shape, dim):
    return lax.broadcasted_iota(jnp.int32, shape, dim)


def one_hot(hit):
    return jnp.where(hit, 1.0, 0.0).astype(BF)


def leaky(v):
    return jnp.maximum(v, 0.2 * v)


def kernel(
    sizes, feat, wts, bias, out,
    raw, wall, ball, f1, f2, fm, fp, h0, hm, hp, tm, ws, base, brow, wbase, pm, ones, xe,
    eb1, eb2, yb1, yb2, hn, res, stage,
    lsem, wsem, wrs, ssx, rsx, ssy, rsy, ssz, rsz, sso, rso,
):
    ngx, ngy = sizes
    seg, gx = lax.axis_index("segment"), lax.axis_index("gx")
    gy, gz = lax.axis_index("gy"), lax.axis_index("gz")
    has = {
        ("x", 1): gx < ngx - 1, ("x", -1): gx > 0,
        ("y", 1): gy < ngy - 1, ("y", -1): gy > 0,
    }
    here = {"x": gx, "y": gy}

    def to(axis, step):
        return {"g" + axis: here[axis] + step}

    lanes = iota((C, L), 1)
    edge = jnp.where(gz == 0, L - 1, 0)
    inner = jnp.where(gz == 0, L - 2, 1)

    load = pltpu.make_async_copy(feat.at[seg], raw, lsem.at[0])
    load.start()
    wl = pltpu.make_async_copy(wts, wall.at[seg], lsem.at[1])
    wl.start()
    bl = pltpu.make_async_copy(bias, ball.at[seg], lsem.at[2])
    bl.start()

    zrow = jnp.zeros((C, L), BF)

    def clear(ref, x0, x1, y0, y1):
        def body(i, c):
            for y in range(y0, y1):
                ref[i, y] = zrow
            return c
        lax.fori_loop(x0, x1, body, 0)

    for f in (f1, f2):
        clear(f, 0, FX, NYL + 4, FY)
        pl.when(gx == 0)(lambda f=f: clear(f, 0, 2, 0, FY))
        pl.when(gx == ngx - 1)(lambda f=f: clear(f, FX - 2, FX, 0, FY))
        pl.when(gy == 0)(lambda f=f: clear(f, 0, FX, 0, 2))
        pl.when(gy == ngy - 1)(lambda f=f: clear(f, 0, FX, NYL + 2, NYL + 4))
    for e in (eb1, eb2):
        for s in range(2):
            for i in range(FX):
                e[s, i] = zrow
    for e in (yb1, yb2):
        for d in range(2):
            for s in range(2):
                for i in range(NXL):
                    e[d, s, i] = zrow

    bar = pltpu.get_barrier_semaphore()
    for (axis, step), ok in has.items():
        @pl.when(ok)
        def _(axis=axis, step=step):
            pl.semaphore_signal(bar, inc=1, device_id=to(axis, step), device_id_type=MESH)
    pl.semaphore_signal(bar, inc=1, device_id={"gz": 1 - gz}, device_id_type=MESH)
    pl.semaphore_signal(bar, inc=1, device_id={"segment": 1 - seg}, device_id_type=MESH)

    r = lax.broadcasted_iota(jnp.int32, (256, 256), 0)
    c = lax.broadcasted_iota(jnp.int32, (256, 256), 1)
    pm[...] = jnp.where((r // 16 == c % 16) & (r % 16 == c // 16), 1.0, 0.0).astype(BF)
    orow = lax.broadcasted_iota(jnp.int32, (L, L), 0)
    ones[...] = jnp.where(orow < C, 1.0, 0.0).astype(BF)
    re, ce = iota((L, L), 0), iota((L, L), 1)
    def table_e(y, carry):
        hit = (re == edge) & (ce == y + 2) | (re == inner) & (ce == y + 66)
        xe[pl.ds(pl.multiple_of(L * y, L), L), :] = one_hot(hit)
        return carry
    lax.fori_loop(0, NYL, table_e, 0)
    load.wait()
    for y in range(NYL // 16):
        for x in range(0, NXL, 2):
            ab = [raw[:, x + k, 16 * y:16 * y + 16, :].reshape(256, L) for k in range(2)]
            t = dots(pm[...], jnp.concatenate(ab, axis=1)).astype(BF)
            for k in range(2):
                f1[x + k + 2, pl.ds(2 + 16 * y, 16)] = t[:, L * k:L * k + L].reshape(16, C, L)

    count = 2 + sum(jnp.where(ok, 1, 0) for ok in has.values())
    pl.semaphore_wait(bar, count)

    def xcopy(q, f, eb, step, k):
        d = 0 if step > 0 else 1
        mv = -NXL * step
        near, far = (FX - 3, FX - 4) if step > 0 else (2, 3)
        lo = FX - 4 if step > 0 else 2
        part = (
            lambda o: f.at[near + o, pl.ds(2, NYL)],
            lambda o: f.at[far + o, pl.ds(2, NYL)],
            lambda o: f.at[pl.ds(lo + o, 2), pl.ds(0, 2)],
            lambda o: f.at[pl.ds(lo + o, 2), pl.ds(NYL + 2, 2)],
            lambda o: eb.at[:, pl.ds(lo + o, 2)],
        )[k]
        return pltpu.make_async_remote_copy(
            part(0), part(mv), ssx.at[q, d, k], rsx.at[q, d, k],
            device_id=to("x", step), device_id_type=MESH)

    def yrows(q, f, step):
        d = 0 if step > 0 else 1
        src, dst = (NYL, 0) if step > 0 else (2, NYL + 2)
        return pltpu.make_async_remote_copy(
            f.at[pl.ds(2, NXL), pl.ds(src, 2)], f.at[pl.ds(2, NXL), pl.ds(dst, 2)],
            ssy.at[q, d, 0], rsy.at[q, d, 0], device_id=to("y", step), device_id_type=MESH)

    def yedges(q, eb, yb, step):
        d = 0 if step > 0 else 1
        return pltpu.make_async_remote_copy(
            eb.at[:, pl.ds(2, NXL)], yb.at[d],
            ssy.at[q, d, 1], rsy.at[q, d, 1], device_id=to("y", step), device_id_type=MESH)

    def zcopy(q, eb):
        return pltpu.make_async_remote_copy(
            eb.at[0, pl.ds(2, NXL)], eb.at[1, pl.ds(2, NXL)], ssz.at[q], rsz.at[q],
            device_id={"gz": 1 - gz}, device_id_type=MESH)

    def ocopy(q):
        return pltpu.make_async_remote_copy(
            stage.at[q], out.at[seg], sso.at[q], rso.at[q],
            device_id={"segment": 1 - seg}, device_id_type=MESH)

    def wcopy(k, ref, sec=seg):
        return pltpu.make_async_remote_copy(
            ref.at[sec], ref.at[sec], wsem.at[k], wrs.at[k],
            device_id={"segment": 1 - seg}, device_id_type=MESH)


    def pack_edges(f, eb):
        acc = None
        for y in range(0, NYL, 2):
            lhs = [f[pl.ds(2, NXL), 2 + y + k].reshape(NXL * C, L) for k in range(2)]
            t = dots(jnp.concatenate(lhs, axis=1), xe[pl.ds(L * y, 2 * L), :])
            acc = t if acc is None else acc + t
        eb[0, pl.ds(2, NXL)] = acc.astype(BF).reshape(NXL, C, L)

    def start_exchange(q, f, eb, yb):
        for step in (1, -1):
            @pl.when(has["x", step])
            def _(step=step):
                xcopy(q, f, eb, step, 0).start()
                xcopy(q, f, eb, step, 1).start()
        for step in (1, -1):
            @pl.when(has["y", step])
            def _(step=step):
                yrows(q, f, step).start()
        pack_edges(f, eb)
        zcopy(q, eb).start()

    def middle_exchange(q, f, eb, yb):
        for step in (1, -1):
            @pl.when(has["y", -step])
            def _(step=step):
                yrows(q, f, step).wait_recv()
        for step in (1, -1):
            @pl.when(has["x", step])
            def _(step=step):
                xcopy(q, f, eb, step, 2).start()
                xcopy(q, f, eb, step, 3).start()
        zcopy(q, eb).wait_recv()
        zcopy(q, eb).wait_send()
        for step in (1, -1):
            @pl.when(has["y", step])
            def _(step=step):
                yedges(q, eb, yb, step).start()
        for step in (1, -1):
            @pl.when(has["y", -step])
            def _(step=step):
                yedges(q, eb, yb, step).wait_recv()
            @pl.when(has["y", step])
            def _(step=step):
                yedges(q, eb, yb, step).wait_send()
        low = lanes % 64
        for s in range(2):
            for x in range(NXL):
                v = eb[s, x + 2]
                v = jnp.where(low < 2, pltpu.roll(yb[0, s, x], L - NYL, 1), v)
                v = jnp.where((low >= NYL + 2) & (low < NYL + 4), pltpu.roll(yb[1, s, x], NYL, 1), v)
                eb[s, x + 2] = v
        for step in (1, -1):
            @pl.when(has["x", step])
            def _(step=step):
                xcopy(q, f, eb, step, 4).start()

    def end_exchange(q, f, eb, yb):
        for step in (1, -1):
            @pl.when(has["x", -step])
            def _(step=step):
                for k in range(5):
                    xcopy(q, f, eb, step, k).wait_recv()
            @pl.when(has["x", step])
            def _(step=step):
                for k in range(5):
                    xcopy(q, f, eb, step, k).wait_send()
            @pl.when(has["y", step])
            def _(step=step):
                yrows(q, f, step).wait_send()

    def make_weights(sec):
        for lay in range(2):
            base[...] = jnp.zeros_like(base)
            for dz in range(3):
                for dx in range(3):
                    for dy in range(3):
                        p = 16 * (dx * 6 + dy)
                        base[dz, :, p:p + 16] = wall[sec, lay, dx * 9 + dy * 3 + dz].astype(F32)
            brow[0:1, 0:C] = ball[sec, lay:lay + 1, :].astype(F32)
            for xq in range(2):
                for yq in range(4):
                    rows = slice(16 * (4 * xq + yq), 16 * (4 * xq + yq) + 16)
                    for dz in range(3):
                        v = base[dz]
                        if 6 * xq + yq:
                            v = pltpu.roll(v, 16 * (6 * xq + yq), 1)
                        tm[2 * sec + lay, rows, 384 * dz:384 * dz + 384] = v.astype(BF)
            br = jnp.broadcast_to(brow[0:1, :], (L, L))
            rr = lax.broadcasted_iota(jnp.int32, (L, L), 0)
            cc = lax.broadcasted_iota(jnp.int32, (L, L), 1)
            diag = jnp.where(rr % 16 == cc, br, 0.0).astype(BF)
            tm[2 * sec + lay, :, 1152:1280] = diag
            if lay == 0:
                wbase[...] = jnp.zeros_like(wbase)
                for dy in range(3):
                    for dx in range(3):
                        for col in range(3):
                            p = 16 * (dx * 3 + col)
                            dz = jnp.where(gz == 0, col, 2 - col)
                            wbase[16 * dy:16 * dy + 16, p:p + 16] = wall[
                                sec, 0, dx * 9 + dy * 3 + dz].astype(F32)
                wbase[16:32, 144:160] = diag[0:16, 0:16].astype(F32)
                ws[sec] = wbase[...].astype(BF)

    def shifted(v, n, lane):
        h = jnp.where(lanes == edge, pltpu.roll(n, (L - lane) % L, 1) if lane else n, zrow)
        return (jnp.where(lanes == 0, h, pltpu.roll(v, 1, 1)),
                jnp.where(lanes == L - 1, h, pltpu.roll(v, L - 1, 1)))

    def shift(f, eb, planes):
        for x in planes:
            n = pltpu.roll(eb[1, x], edge, 1)
            for y in range(NYL + 4):
                fm[x, y], fp[x, y] = shifted(f[x, y], n, y)

    def strips(sec, eb):
        one = ones[0:C, :]
        tail = jnp.zeros((256 - 160, L), BF)
        lane = lax.broadcasted_iota(jnp.int32, (C, L), 1)
        for j in range(HX):
            rows = []
            for dx in range(3):
                rows += [eb[0, j + dx], eb[1, j + dx], pltpu.roll(eb[1, j + dx], 64, 1)]
            m = dots(ws[sec], jnp.concatenate(rows + [one, tail], axis=0))
            v = pltpu.roll(m[0:16], 1, 1) + m[16:32] + pltpu.roll(m[32:48], L - 1, 1)
            v = leaky(v)
            bad = (lane == 1) & (gy == 0) | (lane == NYL + 2) & (gy == ngy - 1)
            if j == 0:
                bad = bad | (gx == 0)
            if j == HX - 1:
                bad = bad | (gx == ngx - 1)
            hn[j] = jnp.where(bad, 0.0, v).astype(BF)

    def boxes(lay, fields, pairs):
        acc = None
        for k in range(5):
            cols = []
            for x0, y0 in pairs:
                rows = []
                for p in range(16 * k, min(16 * k + 16, 72)):
                    g, yr = divmod(p, 6)
                    rows.append(fields[g // 4][x0 + g % 4, y0 + yr])
                if k == 4:
                    rows.append(ones[...])
                cols.append(jnp.concatenate(rows, axis=0))
            t = dots(tm[lay, :, 256 * k:256 * k + 256], jnp.concatenate(cols, axis=1))
            acc = t if acc is None else acc + t
        return leaky(acc).astype(BF)

    def layer_a(sec, f, todo):
        ns = [pltpu.roll(hn[j], edge, 1) for j in range(HX)]
        for h in range(0, len(todo), 2):
            pairs = todo[h:h + 2]
            v = boxes(2 * sec, (fm, f, fp), pairs)
            for k, (x0, y0) in enumerate(pairs):
                b = v[:, L * k:L * k + L].reshape(2, 4, C, L)
                for xq in range(2):
                    for yq in range(4):
                        x, y = x0 + xq, y0 + yq
                        h0[x, y] = b[xq, yq]
                        hm[x, y], hp[x, y] = shifted(b[xq, yq], ns[x], y + 1)
        for r in (h0, hm, hp):
            pl.when(gx == 0)(lambda r=r: clear(r, 0, 1, 0, HY))
            pl.when(gx == ngx - 1)(lambda r=r: clear(r, HX - 1, HX, 0, HY))
            pl.when(gy == 0)(lambda r=r: clear(r, 0, HX, 0, 1))
            pl.when(gy == ngy - 1)(lambda r=r: clear(r, 0, HX, NYL + 1, NYL + 2))

    def layer_b(sec, g, gx0, gy0, todo):
        for h in range(0, len(todo), 2):
            pairs = todo[h:h + 2]
            v = boxes(2 * sec + 1, (hm, h0, hp), pairs)
            for k, (x0, y0) in enumerate(pairs):
                b = v[:, L * k:L * k + L].reshape(2, 4, C, L)
                for xq in range(2):
                    g[gx0 + x0 + xq, pl.ds(gy0 + y0, 4)] = b[xq]

    def channels_first(g, gx0, gy0, dst):
        for y in range(NYL // 16):
            for x in range(0, NXL, 2):
                ab = [g[gx0 + x + k, pl.ds(gy0 + 16 * y, 16)].reshape(256, L) for k in range(2)]
                t = dots(pm[...], jnp.concatenate(ab, axis=1)).astype(BF)
                for k in range(2):
                    dst[:, x + k, 16 * y:16 * y + 16, :] = t[:, L * k:L * k + L].reshape(C, 16, L)

    def send_out(q, g, gx0, gy0):
        @pl.when(seg == q)
        def _():
            channels_first(g, gx0, gy0, out.at[seg])
        @pl.when(seg != q)
        def _():
            channels_first(g, gx0, gy0, stage.at[q])
            ocopy(q).start()

    def boxes_of(xs, ny):
        return [(x, y) for y in range(0, ny, 4) for x in xs]

    start_exchange(0, f1, eb1, yb1)
    wl.wait()
    bl.wait()
    wcopy(0, wall).start()
    wcopy(1, ball).start()
    middle_exchange(0, f1, eb1, yb1)
    brow[...] = jnp.zeros_like(brow)
    wcopy(0, wall, 1 - seg).wait_recv()
    wcopy(1, ball, 1 - seg).wait_recv()
    wcopy(0, wall).wait_send()
    wcopy(1, ball).wait_send()
    for f in (fm, fp):
        clear(f, 0, FX, NYL + 4, FY)
    for sec in range(2):
        make_weights(sec)
    end_exchange(0, f1, eb1, yb1)

    shift(f1, eb1, range(FX))
    strips(0, eb1)
    layer_a(0, f1, boxes_of((0, 2, 4), HY))
    layer_b(0, f2, 2, 2, boxes_of((0, 2), NYL))

    start_exchange(1, f2, eb2, yb2)
    send_out(0, f2, 2, 2)
    middle_exchange(1, f2, eb2, yb2)
    end_exchange(1, f2, eb2, yb2)

    shift(f2, eb2, range(FX))
    strips(1, eb2)
    layer_a(1, f2, boxes_of((0, 2, 4), HY))
    layer_b(1, res, 0, 0, boxes_of((0, 2), NYL))
    send_out(1, res, 0, 0)

    for q in range(2):
        @pl.when(seg == q)
        def _(q=q):
            pltpu.make_async_remote_copy(
                stage.at[q], out.at[1 - seg], sso.at[q], rso.at[q],
                device_id={"segment": 1 - seg}, device_id_type=MESH).wait_recv()
        @pl.when(seg != q)
        def _(q=q):
            ocopy(q).wait_send()


def shards(sizes, features, weights, biases):
    w = weights[0].transpose(0, 3, 4, 5, 1, 2).reshape(2, 27, C, C)
    hbm = pl.BlockSpec(memory_space=pltpu.HBM)
    dma = pltpu.SemaphoreType.DMA
    out = pl.pallas_call(
        functools.partial(kernel, sizes),
        name="sections",
        out_shape=jax.ShapeDtypeStruct((2, C, NXL, NYL, L), BF),
        in_specs=[hbm] * 3,
        out_specs=pl.BlockSpec(memory_space=pltpu.VMEM),
        scratch_shapes=[
            pltpu.VMEM((C, NXL, NYL, L), BF),
            pltpu.VMEM((2, 2, 27, C, C), BF),
            pltpu.VMEM((2, 2, C), BF),
            pltpu.VMEM((FX, FY, C, L), BF),
            pltpu.VMEM((FX, FY, C, L), BF),
            pltpu.VMEM((FX, FY, C, L), BF),
            pltpu.VMEM((FX, FY, C, L), BF),
            pltpu.VMEM((HX, HY, C, L), BF),
            pltpu.VMEM((HX, HY, C, L), BF),
            pltpu.VMEM((HX, HY, C, L), BF),
            pltpu.VMEM((4, L, KT), BF),
            pltpu.VMEM((2, 48, 256), BF),
            pltpu.VMEM((3, C, 384), F32),
            pltpu.VMEM((8, L), F32),
            pltpu.VMEM((48, 256), F32),
            pltpu.VMEM((256, 256), BF),
            pltpu.VMEM((L, L), BF),
            pltpu.VMEM((NYL * L, L), BF),
            pltpu.VMEM((2, FX, C, L), BF),
            pltpu.VMEM((2, FX, C, L), BF),
            pltpu.VMEM((2, 2, NXL, C, L), BF),
            pltpu.VMEM((2, 2, NXL, C, L), BF),
            pltpu.VMEM((HX, C, L), BF),
            pltpu.VMEM((NXL, NYL, C, L), BF),
            pltpu.VMEM((2, C, NXL, NYL, L), BF),
            dma((3,)), dma((2,)), dma((2,)),
            dma((2, 2, 5)), dma((2, 2, 5)),
            dma((2, 2, 2)), dma((2, 2, 2)),
            dma((2,)), dma((2,)), dma((2,)), dma((2,)),
        ],
        compiler_params=pltpu.CompilerParams(
            collective_id=0, has_side_effects=True, vmem_limit_bytes=32 << 20),
    )(*(pltpu.with_memory_space_constraint(a, pltpu.HBM) for a in (features, w, biases[0])))
    return out[None]


def solution(mesh):
    placed = (
        P(None, None, "gx", "gy", "gz"),
        P("segment", None, None, None, None, None, None),
        P("segment", None, None),
    )
    sizes = (mesh.shape["gx"], mesh.shape["gy"])
    return jax.shard_map(
        functools.partial(shards, sizes),
        mesh=mesh,
        in_specs=placed,
        out_specs=P("segment", None, None, "gx", "gy", "gz"),
        check_vma=False,
    )
```

```python
import functools

import jax
import jax.numpy as jnp
from jax import lax
from jax.experimental import pallas as pl
from jax.experimental.pallas import tpu as pltpu
from jax.sharding import PartitionSpec as P

MESH = pl.DeviceIdType.MESH
BF = jnp.bfloat16
F32 = jnp.float32

NXL, NYL, C, L = 4, 32, 16, 128
FX, FY = NXL + 4, NYL + 6
HX, HY = NXL + 2, NYL + 4
KT = 1280


def dots(a, b):
    return jnp.dot(a, b, preferred_element_type=F32)


def iota(shape, dim):
    return lax.broadcasted_iota(jnp.int32, shape, dim)


def one_hot(hit):
    return jnp.where(hit, 1.0, 0.0).astype(BF)


def leaky(v):
    return jnp.maximum(v, 0.2 * v)


def kernel(
    sizes, feat, wts, bias, out,
    raw, wall, ball, f1, f2, fm, fp, h0, hm, hp, tm, ws, base, brow, wbase, pm, ones, xe,
    eb1, eb2, yb1, yb2, hn, res, stage,
    lsem, wsem, wrs, ssx, rsx, ssy, rsy, sse, rse, ssz, rsz, sso, rso,
):
    ngx, ngy = sizes
    seg, gx = lax.axis_index("segment"), lax.axis_index("gx")
    gy, gz = lax.axis_index("gy"), lax.axis_index("gz")
    has = {
        ("x", 1): gx < ngx - 1, ("x", -1): gx > 0,
        ("y", 1): gy < ngy - 1, ("y", -1): gy > 0,
    }
    here = {"x": gx, "y": gy}

    def to(axis, step):
        return {"g" + axis: here[axis] + step}

    lanes = iota((C, L), 1)
    edge = jnp.where(gz == 0, L - 1, 0)
    inner = jnp.where(gz == 0, L - 2, 1)

    load = pltpu.make_async_copy(feat.at[seg], raw, lsem.at[0])
    load.start()
    wl = pltpu.make_async_copy(wts, wall.at[seg], lsem.at[1])
    wl.start()
    bl = pltpu.make_async_copy(bias, ball.at[seg], lsem.at[2])
    bl.start()

    zrow = jnp.zeros((C, L), BF)

    def clear(ref, x0, x1, y0, y1):
        def body(i, c):
            for y in range(y0, y1):
                ref[i, y] = zrow
            return c
        lax.fori_loop(x0, x1, body, 0)

    for f in (f1, f2):
        clear(f, 0, FX, NYL + 4, FY)
        pl.when(gx == 0)(lambda f=f: clear(f, 0, 2, 0, FY))
        pl.when(gx == ngx - 1)(lambda f=f: clear(f, FX - 2, FX, 0, FY))
        pl.when(gy == 0)(lambda f=f: clear(f, 0, FX, 0, 2))
        pl.when(gy == ngy - 1)(lambda f=f: clear(f, 0, FX, NYL + 2, NYL + 4))
    for e in (eb1, eb2):
        for s in range(2):
            for i in range(FX):
                e[s, i] = zrow
    for e in (yb1, yb2):
        for d in range(2):
            for s in range(2):
                for i in range(NXL):
                    e[d, s, i] = zrow

    bar = pltpu.get_barrier_semaphore()
    for (axis, step), ok in has.items():
        @pl.when(ok)
        def _(axis=axis, step=step):
            pl.semaphore_signal(bar, inc=1, device_id=to(axis, step), device_id_type=MESH)
            if axis == "y":
                pl.semaphore_signal(
                    bar, inc=1, device_id={"gy": gy + step, "gz": 1 - gz}, device_id_type=MESH)
    pl.semaphore_signal(bar, inc=1, device_id={"gz": 1 - gz}, device_id_type=MESH)
    pl.semaphore_signal(bar, inc=1, device_id={"segment": 1 - seg}, device_id_type=MESH)

    r = lax.broadcasted_iota(jnp.int32, (256, 256), 0)
    c = lax.broadcasted_iota(jnp.int32, (256, 256), 1)
    pm[...] = jnp.where((r // 16 == c % 16) & (r % 16 == c // 16), 1.0, 0.0).astype(BF)
    orow = lax.broadcasted_iota(jnp.int32, (L, L), 0)
    ones[...] = jnp.where(orow < C, 1.0, 0.0).astype(BF)
    re, ce = iota((L, L), 0), iota((L, L), 1)
    def table_e(y, carry):
        hit = (re == edge) & (ce == y + 2) | (re == inner) & (ce == y + 66)
        xe[pl.ds(pl.multiple_of(L * y, L), L), :] = one_hot(hit)
        return carry
    lax.fori_loop(0, NYL, table_e, 0)
    load.wait()
    for y in range(NYL // 16):
        for x in range(0, NXL, 2):
            ab = [raw[:, x + k, 16 * y:16 * y + 16, :].reshape(256, L) for k in range(2)]
            t = dots(pm[...], jnp.concatenate(ab, axis=1)).astype(BF)
            for k in range(2):
                f1[x + k + 2, pl.ds(2 + 16 * y, 16)] = t[:, L * k:L * k + L].reshape(16, C, L)

    count = 2 + sum(
        jnp.where(ok, 2 if axis == "y" else 1, 0) for (axis, _), ok in has.items())
    pl.semaphore_wait(bar, count)

    def xcopy(q, f, eb, step, half, k):
        d = 0 if step > 0 else 1
        mv = -NXL * step
        src = (FX - 3, FX - 4)[half] if step > 0 else (2, 3)[half]
        part = (
            lambda x: f.at[x, pl.ds(2, NYL)],
            lambda x: f.at[x, pl.ds(0, 2)],
            lambda x: f.at[x, pl.ds(NYL + 2, 2)],
            lambda x: eb.at[:, x],
        )[k]
        return pltpu.make_async_remote_copy(
            part(src), part(src + mv), ssx.at[q, d, half, k], rsx.at[q, d, half, k],
            device_id=to("x", step), device_id_type=MESH)

    def yrows(q, f, step, p):
        d = 0 if step > 0 else 1
        src, dst = (NYL, 0) if step > 0 else (2, NYL + 2)
        return pltpu.make_async_remote_copy(
            f.at[2 + p, pl.ds(src, 2)], f.at[2 + p, pl.ds(dst, 2)],
            ssy.at[q, d, p], rsy.at[q, d, p], device_id=to("y", step), device_id_type=MESH)

    def yedges(q, eb, yb, step, other, p):
        d = 0 if step > 0 else 1
        return pltpu.make_async_remote_copy(
            eb.at[0, 2 + p], yb.at[d, other, p],
            sse.at[q, d, other, p], rse.at[q, d, other, p],
            device_id={"gy": gy + step, "gz": 1 - gz if other else gz}, device_id_type=MESH)

    def zcopy(q, eb, p):
        return pltpu.make_async_remote_copy(
            eb.at[0, 2 + p], eb.at[1, 2 + p], ssz.at[q, p], rsz.at[q, p],
            device_id={"gz": 1 - gz}, device_id_type=MESH)

    def ocopy(q):
        return pltpu.make_async_remote_copy(
            stage.at[q], out.at[seg], sso.at[q], rso.at[q],
            device_id={"segment": 1 - seg}, device_id_type=MESH)

    def wcopy(k, ref, sec=seg):
        return pltpu.make_async_remote_copy(
            ref.at[sec], ref.at[sec], wsem.at[k], wrs.at[k],
            device_id={"segment": 1 - seg}, device_id_type=MESH)


    def pack_edges(f, eb, planes):
        acc = None
        for y in range(0, NYL, 2):
            lhs = [jnp.concatenate([f[2 + p, 2 + y + k] for p in planes], axis=0) for k in range(2)]
            t = dots(jnp.concatenate(lhs, axis=1), xe[pl.ds(L * y, 2 * L), :])
            acc = t if acc is None else acc + t
        acc = acc.astype(BF)
        for i, p in enumerate(planes):
            eb[0, 2 + p] = acc[C * i:C * i + C]

    def each(axis, turn, work):
        for step in (1, -1):
            pl.when(has[axis, turn * step])(lambda step=step: work(step))

    def start_faces(q, f, eb, half):
        each("x", 1, lambda step: xcopy(q, f, eb, step, half, 0).start())

    def start_sides(q, f, eb, yb, planes):
        def rows(step):
            for p in planes:
                yrows(q, f, step, p).start()
        each("y", 1, rows)
        pack_edges(f, eb, planes)
        for p in planes:
            zcopy(q, eb, p).start()
        def strips_out(step):
            for p in planes:
                for other in range(2):
                    yedges(q, eb, yb, step, other, p).start()
        each("y", 1, strips_out)

    def pass_on(q, f, eb, yb, planes, half):
        def rows_in(step):
            for p in planes:
                yrows(q, f, step, p).wait_recv()
        each("y", -1, rows_in)
        def rows_on(step):
            xcopy(q, f, eb, step, half, 1).start()
            xcopy(q, f, eb, step, half, 2).start()
        each("x", 1, rows_on)
        for p in planes:
            zcopy(q, eb, p).wait_recv()
            zcopy(q, eb, p).wait_send()
        def strips_in(step):
            for p in planes:
                for other in range(2):
                    yedges(q, eb, yb, step, other, p).wait_recv()
        each("y", -1, strips_in)
        def strips_gone(step):
            for p in planes:
                for other in range(2):
                    yedges(q, eb, yb, step, other, p).wait_send()
        each("y", 1, strips_gone)
        low = lanes % 64
        for s in range(2):
            for p in planes:
                v = eb[s, p + 2]
                v = jnp.where(low < 2, pltpu.roll(yb[0, s, p], L - NYL, 1), v)
                v = jnp.where((low >= NYL + 2) & (low < NYL + 4), pltpu.roll(yb[1, s, p], NYL, 1), v)
                eb[s, p + 2] = v
        each("x", 1, lambda step: xcopy(q, f, eb, step, half, 3).start())

    def arrive(q, f, eb, half):
        def come(step):
            for k in range(4):
                xcopy(q, f, eb, step, half, k).wait_recv()
        each("x", -1, come)

    def drain(q, f, eb):
        def xgone(step):
            for half in range(2):
                for k in range(4):
                    xcopy(q, f, eb, step, half, k).wait_send()
        each("x", 1, xgone)
        def ygone(step):
            for p in range(NXL):
                yrows(q, f, step, p).wait_send()
        each("y", 1, ygone)

    def make_weights(sec):
        for lay in range(2):
            base[...] = jnp.zeros_like(base)
            for dz in range(3):
                for dx in range(3):
                    for dy in range(3):
                        p = 16 * (dx * 6 + dy)
                        base[dz, :, p:p + 16] = wall[sec, lay, dx * 9 + dy * 3 + dz].astype(F32)
            brow[0:1, 0:C] = ball[sec, lay:lay + 1, :].astype(F32)
            for xq in range(2):
                for yq in range(4):
                    rows = slice(16 * (4 * xq + yq), 16 * (4 * xq + yq) + 16)
                    for dz in range(3):
                        v = base[dz]
                        if 6 * xq + yq:
                            v = pltpu.roll(v, 16 * (6 * xq + yq), 1)
                        tm[2 * sec + lay, rows, 384 * dz:384 * dz + 384] = v.astype(BF)
            br = jnp.broadcast_to(brow[0:1, :], (L, L))
            rr = lax.broadcasted_iota(jnp.int32, (L, L), 0)
            cc = lax.broadcasted_iota(jnp.int32, (L, L), 1)
            diag = jnp.where(rr % 16 == cc, br, 0.0).astype(BF)
            tm[2 * sec + lay, :, 1152:1280] = diag
            if lay == 0:
                wbase[...] = jnp.zeros_like(wbase)
                for dy in range(3):
                    for dx in range(3):
                        for col in range(3):
                            p = 16 * (dx * 3 + col)
                            dz = jnp.where(gz == 0, col, 2 - col)
                            wbase[16 * dy:16 * dy + 16, p:p + 16] = wall[
                                sec, 0, dx * 9 + dy * 3 + dz].astype(F32)
                wbase[16:32, 144:160] = diag[0:16, 0:16].astype(F32)
                ws[sec] = wbase[...].astype(BF)

    def shifted(v, n, lane):
        h = jnp.where(lanes == edge, pltpu.roll(n, (L - lane) % L, 1) if lane else n, zrow)
        return (jnp.where(lanes == 0, h, pltpu.roll(v, 1, 1)),
                jnp.where(lanes == L - 1, h, pltpu.roll(v, L - 1, 1)))

    def shift(f, eb, planes):
        for x in planes:
            n = pltpu.roll(eb[1, x], edge, 1)
            for y in range(NYL + 4):
                fm[x, y], fp[x, y] = shifted(f[x, y], n, y)

    def strips(sec, eb, todo):
        one = ones[0:C, :]
        tail = jnp.zeros((256 - 160, L), BF)
        lane = lax.broadcasted_iota(jnp.int32, (C, L), 1)
        for j in todo:
            rows = []
            for dx in range(3):
                rows += [eb[0, j + dx], eb[1, j + dx], pltpu.roll(eb[1, j + dx], 64, 1)]
            m = dots(ws[sec], jnp.concatenate(rows + [one, tail], axis=0))
            v = pltpu.roll(m[0:16], 1, 1) + m[16:32] + pltpu.roll(m[32:48], L - 1, 1)
            v = leaky(v)
            bad = (lane == 1) & (gy == 0) | (lane == NYL + 2) & (gy == ngy - 1)
            if j == 0:
                bad = bad | (gx == 0)
            if j == HX - 1:
                bad = bad | (gx == ngx - 1)
            hn[j] = jnp.where(bad, 0.0, v).astype(BF)

    def boxes(lay, fields, pairs, xqs):
        acc = None
        for k in range(5):
            cols = []
            for x0, y0 in pairs:
                rows = []
                for p in range(16 * k, min(16 * k + 16, 72)):
                    g, yr = divmod(p, 6)
                    rows.append(fields[g // 4][x0 + g % 4, y0 + yr])
                if k == 4:
                    rows.append(ones[...])
                cols.append(jnp.concatenate(rows, axis=0))
            t = dots(tm[lay, 64 * xqs[0]:64 * xqs[-1] + 64, 256 * k:256 * k + 256], jnp.concatenate(cols, axis=1))
            acc = t if acc is None else acc + t
        return leaky(acc).astype(BF)

    def layer(lay, fields, todo, xqs, put):
        for h in range(0, len(todo), 2):
            pairs = todo[h:h + 2]
            v = boxes(lay, fields, pairs, xqs)
            for k, (x0, y0) in enumerate(pairs):
                b = v[:, L * k:L * k + L].reshape(len(xqs), 4, C, L)
                for i, xq in enumerate(xqs):
                    for yq in range(4):
                        put(x0 + xq, y0 + yq, b[i, yq])

    def layer_a(sec, f, todo, xqs=(0, 1)):
        xs = sorted({x0 + xq for x0, _ in todo for xq in xqs})
        ns = {x: pltpu.roll(hn[x], edge, 1) for x in xs}
        def put(x, y, t):
            h0[x, y] = t
            hm[x, y], hp[x, y] = shifted(t, ns[x], y + 1)
        layer(2 * sec, (fm, f, fp), todo, xqs, put)

    def outside():
        for r in (h0, hm, hp):
            pl.when(gx == 0)(lambda r=r: clear(r, 0, 1, 0, HY))
            pl.when(gx == ngx - 1)(lambda r=r: clear(r, HX - 1, HX, 0, HY))
            pl.when(gy == 0)(lambda r=r: clear(r, 0, HX, 0, 1))
            pl.when(gy == ngy - 1)(lambda r=r: clear(r, 0, HX, NYL + 1, NYL + 2))

    def layer_b(sec, g, o, todo, xqs=(0, 1)):
        def put(x, y, t):
            g[o + x, o + y] = t
        layer(2 * sec + 1, (hm, h0, hp), todo, xqs, put)

    def channels_first(g, gx0, gy0, dst):
        for y in range(NYL // 16):
            for x in range(0, NXL, 2):
                ab = [g[gx0 + x + k, pl.ds(gy0 + 16 * y, 16)].reshape(256, L) for k in range(2)]
                t = dots(pm[...], jnp.concatenate(ab, axis=1)).astype(BF)
                for k in range(2):
                    dst[:, x + k, 16 * y:16 * y + 16, :] = t[:, L * k:L * k + L].reshape(C, 16, L)

    def send_out(q, g, gx0, gy0):
        @pl.when(seg == q)
        def _():
            channels_first(g, gx0, gy0, out.at[seg])
        @pl.when(seg != q)
        def _():
            channels_first(g, gx0, gy0, stage.at[q])
            ocopy(q).start()

    def boxes_of(xs, ny):
        return [(x, y) for y in range(0, ny, 4) for x in xs]

    near, far = (0, 3), (1, 2)
    start_faces(0, f1, eb1, 0)
    start_sides(0, f1, eb1, yb1, (0, 1, 2, 3))
    wl.wait()
    bl.wait()
    wcopy(0, wall).start()
    wcopy(1, ball).start()
    pass_on(0, f1, eb1, yb1, near, 0)
    start_faces(0, f1, eb1, 1)
    pass_on(0, f1, eb1, yb1, far, 1)
    brow[...] = jnp.zeros_like(brow)
    wcopy(0, wall, 1 - seg).wait_recv()
    wcopy(1, ball, 1 - seg).wait_recv()
    wcopy(0, wall).wait_send()
    wcopy(1, ball).wait_send()
    for f in (fm, fp):
        clear(f, 0, FX, NYL + 4, FY)
    for sec in range(2):
        make_weights(sec)

    arrive(0, f1, eb1, 0)
    shift(f1, eb1, range(1, FX - 1))
    strips(0, eb1, range(1, HX - 1))
    layer_a(0, f1, boxes_of((1, 3), HY))
    outside()
    layer_b(0, f2, 2, boxes_of((1,), NYL))
    start_faces(1, f2, eb2, 1)
    start_sides(1, f2, eb2, yb2, far)
    arrive(0, f1, eb1, 1)
    shift(f1, eb1, (0, FX - 1))
    strips(0, eb1, (0, HX - 1))
    layer_a(0, f1, boxes_of((0,), HY), (0,))
    layer_a(0, f1, boxes_of((4,), HY), (1,))
    outside()
    layer_b(0, f2, 2, boxes_of((0,), NYL), (0,))
    layer_b(0, f2, 2, boxes_of((2,), NYL), (1,))

    start_faces(1, f2, eb2, 0)
    start_sides(1, f2, eb2, yb2, near)
    send_out(0, f2, 2, 2)
    pass_on(1, f2, eb2, yb2, far, 1)
    pass_on(1, f2, eb2, yb2, near, 0)
    shift(f2, eb2, range(2, FX - 2))
    strips(1, eb2, (2, 3))
    layer_a(1, f2, boxes_of((2,), HY))
    arrive(1, f2, eb2, 1)
    shift(f2, eb2, (0, FX - 1))
    arrive(1, f2, eb2, 0)
    shift(f2, eb2, (1, FX - 2))
    strips(1, eb2, (0, 1, 4, 5))
    layer_a(1, f2, boxes_of((0, 4), HY))
    outside()
    layer_b(1, res, 0, boxes_of((0, 2), NYL))
    send_out(1, res, 0, 0)
    drain(0, f1, eb1)
    drain(1, f2, eb2)

    for q in range(2):
        @pl.when(seg == q)
        def _(q=q):
            pltpu.make_async_remote_copy(
                stage.at[q], out.at[1 - seg], sso.at[q], rso.at[q],
                device_id={"segment": 1 - seg}, device_id_type=MESH).wait_recv()
        @pl.when(seg != q)
        def _(q=q):
            ocopy(q).wait_send()


def shards(sizes, features, weights, biases):
    w = weights[0].transpose(0, 3, 4, 5, 1, 2).reshape(2, 27, C, C)
    hbm = pl.BlockSpec(memory_space=pltpu.HBM)
    dma = pltpu.SemaphoreType.DMA
    out = pl.pallas_call(
        functools.partial(kernel, sizes),
        name="sections",
        out_shape=jax.ShapeDtypeStruct((2, C, NXL, NYL, L), BF),
        in_specs=[hbm] * 3,
        out_specs=pl.BlockSpec(memory_space=pltpu.VMEM),
        scratch_shapes=[
            pltpu.VMEM((C, NXL, NYL, L), BF),
            pltpu.VMEM((2, 2, 27, C, C), BF),
            pltpu.VMEM((2, 2, C), BF),
            pltpu.VMEM((FX, FY, C, L), BF),
            pltpu.VMEM((FX, FY, C, L), BF),
            pltpu.VMEM((FX, FY, C, L), BF),
            pltpu.VMEM((FX, FY, C, L), BF),
            pltpu.VMEM((HX, HY, C, L), BF),
            pltpu.VMEM((HX, HY, C, L), BF),
            pltpu.VMEM((HX, HY, C, L), BF),
            pltpu.VMEM((4, L, KT), BF),
            pltpu.VMEM((2, 48, 256), BF),
            pltpu.VMEM((3, C, 384), F32),
            pltpu.VMEM((8, L), F32),
            pltpu.VMEM((48, 256), F32),
            pltpu.VMEM((256, 256), BF),
            pltpu.VMEM((L, L), BF),
            pltpu.VMEM((NYL * L, L), BF),
            pltpu.VMEM((2, FX, C, L), BF),
            pltpu.VMEM((2, FX, C, L), BF),
            pltpu.VMEM((2, 2, NXL, C, L), BF),
            pltpu.VMEM((2, 2, NXL, C, L), BF),
            pltpu.VMEM((HX, C, L), BF),
            pltpu.VMEM((NXL, NYL, C, L), BF),
            pltpu.VMEM((2, C, NXL, NYL, L), BF),
            dma((3,)), dma((2,)), dma((2,)),
            dma((2, 2, 2, 4)), dma((2, 2, 2, 4)),
            dma((2, 2, NXL)), dma((2, 2, NXL)),
            dma((2, 2, 2, NXL)), dma((2, 2, 2, NXL)),
            dma((2, NXL)), dma((2, NXL)), dma((2,)), dma((2,)),
        ],
        compiler_params=pltpu.CompilerParams(
            collective_id=0, has_side_effects=True, vmem_limit_bytes=32 << 20),
    )(*(pltpu.with_memory_space_constraint(a, pltpu.HBM) for a in (features, w, biases[0])))
    return out[None]


def solution(mesh):
    placed = (
        P(None, None, "gx", "gy", "gz"),
        P("segment", None, None, None, None, None, None),
        P("segment", None, None),
    )
    sizes = (mesh.shape["gx"], mesh.shape["gy"])
    return jax.shard_map(
        functools.partial(shards, sizes),
        mesh=mesh,
        in_specs=placed,
        out_specs=P("segment", None, None, "gx", "gy", "gz"),
        check_vma=False,
    )
```

```python
import functools

import jax
import jax.numpy as jnp
from jax import lax
from jax.experimental import pallas as pl
from jax.experimental.pallas import tpu as pltpu
from jax.sharding import PartitionSpec as P

MESH = pl.DeviceIdType.MESH
BF = jnp.bfloat16
F32 = jnp.float32

NXL, NYL, C, L = 4, 32, 16, 128
FX, FY = NXL + 4, NYL + 6
HX, HY = NXL + 2, NYL + 4
CUT = (20, 16)
KT = 1280


def dots(a, b):
    return jnp.dot(a, b, preferred_element_type=F32)


def iota(shape, dim):
    return lax.broadcasted_iota(jnp.int32, shape, dim)


def one_hot(hit):
    return jnp.where(hit, 1.0, 0.0).astype(BF)


def leaky(v):
    return jnp.maximum(v, 0.2 * v)


def kernel(
    sizes, feat, wts, bias, out,
    raw, wall, ball, f1, f2, fm, fp, h0, hm, hp, tm, ws, base, brow, wbase, pm, ones, xe,
    eb1, eb2, yb1, yb2, hn, res, stage,
    lsem, wsem, wrs, ssx, rsx, ssy, rsy, sse, rse, ssz, rsz, sso, rso, osem,
):
    ngx, ngy = sizes
    seg, gx = lax.axis_index("segment"), lax.axis_index("gx")
    gy, gz = lax.axis_index("gy"), lax.axis_index("gz")
    has = {
        ("x", 1): gx < ngx - 1, ("x", -1): gx > 0,
        ("y", 1): gy < ngy - 1, ("y", -1): gy > 0,
    }
    here = {"x": gx, "y": gy}

    def to(axis, step):
        return {"g" + axis: here[axis] + step}

    lanes = iota((C, L), 1)
    edge = jnp.where(gz == 0, L - 1, 0)
    inner = jnp.where(gz == 0, L - 2, 1)

    load = pltpu.make_async_copy(feat.at[seg], raw, lsem.at[0])
    load.start()
    wl = pltpu.make_async_copy(wts, wall.at[seg], lsem.at[1])
    wl.start()
    bl = pltpu.make_async_copy(bias, ball.at[seg], lsem.at[2])
    bl.start()

    zrow = jnp.zeros((C, L), BF)

    def clear(ref, x0, x1, y0, y1):
        def body(i, c):
            for y in range(y0, y1):
                ref[i, y] = zrow
            return c
        lax.fori_loop(x0, x1, body, 0)

    def clear_strips(eb, yb, planes, d):
        for p in planes:
            eb[0, p] = zrow
            eb[1, p] = zrow
        if d is not None:
            for p in range(NXL):
                yb[d, 0, p] = zrow
                yb[d, 1, p] = zrow

    for f, eb, yb in ((f1, eb1, yb1), (f2, eb2, yb2)):
        @pl.when(gx == 0)
        def _(f=f, eb=eb, yb=yb):
            clear(f, 0, 2, 0, NYL + 4)
            clear_strips(eb, yb, (0, 1), None)
        @pl.when(gx == ngx - 1)
        def _(f=f, eb=eb, yb=yb):
            clear(f, FX - 2, FX, 0, NYL + 4)
            clear_strips(eb, yb, (FX - 2, FX - 1), None)
        @pl.when(gy == 0)
        def _(f=f, eb=eb, yb=yb):
            clear(f, 0, FX, 0, 2)
            clear_strips(eb, yb, (), 0)
        @pl.when(gy == ngy - 1)
        def _(f=f, eb=eb, yb=yb):
            clear(f, 0, FX, NYL + 2, NYL + 4)
            clear_strips(eb, yb, (), 1)

    bar = pltpu.get_barrier_semaphore()
    for (axis, step), ok in has.items():
        @pl.when(ok)
        def _(axis=axis, step=step):
            pl.semaphore_signal(bar, inc=1, device_id=to(axis, step), device_id_type=MESH)
            if axis == "y":
                pl.semaphore_signal(
                    bar, inc=1, device_id={"gy": gy + step, "gz": 1 - gz}, device_id_type=MESH)
    pl.semaphore_signal(bar, inc=1, device_id={"gz": 1 - gz}, device_id_type=MESH)
    pl.semaphore_signal(bar, inc=1, device_id={"segment": 1 - seg}, device_id_type=MESH)

    r = lax.broadcasted_iota(jnp.int32, (256, 256), 0)
    c = lax.broadcasted_iota(jnp.int32, (256, 256), 1)
    pm[...] = jnp.where((r // 16 == c % 16) & (r % 16 == c // 16), 1.0, 0.0).astype(BF)
    orow = lax.broadcasted_iota(jnp.int32, (L, L), 0)
    ones[...] = jnp.where(orow < C, 1.0, 0.0).astype(BF)
    re, ce = iota((L, L), 0), iota((L, L), 1)
    def table_e(y, carry):
        hit = (re == edge) & (ce == y + 2) | (re == inner) & (ce == y + 66)
        xe[pl.ds(pl.multiple_of(L * y, L), L), :] = one_hot(hit)
        return carry
    lax.fori_loop(0, NYL, table_e, 0)
    load.wait()
    for y in range(NYL // 16):
        for x in range(0, NXL, 2):
            ab = [raw[:, x + k, 16 * y:16 * y + 16, :].reshape(256, L) for k in range(2)]
            t = dots(pm[...], jnp.concatenate(ab, axis=1)).astype(BF)
            for k in range(2):
                f1[x + k + 2, pl.ds(2 + 16 * y, 16)] = t[:, L * k:L * k + L].reshape(16, C, L)

    count = 2 + sum(
        jnp.where(ok, 2 if axis == "y" else 1, 0) for (axis, _), ok in has.items())
    pl.semaphore_wait(bar, count)

    def xcopy(q, f, eb, step, half, k):
        d = 0 if step > 0 else 1
        mv = -NXL * step
        src = (FX - 3, FX - 4)[half] if step > 0 else (2, 3)[half]
        part = (
            lambda x: f.at[x, pl.ds(2, CUT[q])],
            lambda x: f.at[x, pl.ds(0, 2)],
            lambda x: f.at[x, pl.ds(NYL + 2, 2)],
            lambda x: eb.at[:, x],
            lambda x: f.at[x, pl.ds(2 + CUT[q], NYL - CUT[q])],
        )[k]
        return pltpu.make_async_remote_copy(
            part(src), part(src + mv), ssx.at[q, d, half, k], rsx.at[q, d, half, k],
            device_id=to("x", step), device_id_type=MESH)

    def yrows(q, f, step, p):
        d = 0 if step > 0 else 1
        src, dst = (NYL, 0) if step > 0 else (2, NYL + 2)
        return pltpu.make_async_remote_copy(
            f.at[2 + p, pl.ds(src, 2)], f.at[2 + p, pl.ds(dst, 2)],
            ssy.at[q, d, p], rsy.at[q, d, p], device_id=to("y", step), device_id_type=MESH)

    def yedges(q, eb, yb, step, other, p):
        d = 0 if step > 0 else 1
        return pltpu.make_async_remote_copy(
            eb.at[0, 2 + p], yb.at[d, other, p],
            sse.at[q, d, other, p], rse.at[q, d, other, p],
            device_id={"gy": gy + step, "gz": 1 - gz if other else gz}, device_id_type=MESH)

    def zcopy(q, eb, p):
        return pltpu.make_async_remote_copy(
            eb.at[0, 2 + p], eb.at[1, 2 + p], ssz.at[q, p], rsz.at[q, p],
            device_id={"gz": 1 - gz}, device_id_type=MESH)

    def piece(ref, x, y):
        return ref.at[:, pl.ds(x, 2), pl.ds(y, 16)]

    def ocopy(q, x, y, slot=seg):
        n = x // 2 + y // 8
        return pltpu.make_async_remote_copy(
            piece(stage.at[q], x, y), piece(out.at[slot], x, y), sso.at[q, n], rso.at[q, n],
            device_id={"segment": 1 - seg}, device_id_type=MESH)

    def lcopy(q, x, y):
        return pltpu.make_async_copy(
            piece(stage.at[q], x, y), piece(out.at[seg], x, y), osem.at[q, x // 2 + y // 8])

    def wcopy(k, ref, sec=seg):
        return pltpu.make_async_remote_copy(
            ref.at[sec], ref.at[sec], wsem.at[k], wrs.at[k],
            device_id={"segment": 1 - seg}, device_id_type=MESH)


    def pack_edges(f, eb, planes):
        acc = None
        for y in range(0, NYL, 2):
            lhs = [jnp.concatenate([f[2 + p, 2 + y + k] for p in planes], axis=0) for k in range(2)]
            t = dots(jnp.concatenate(lhs, axis=1), xe[pl.ds(L * y, 2 * L), :])
            acc = t if acc is None else acc + t
        acc = acc.astype(BF)
        for i, p in enumerate(planes):
            eb[0, 2 + p] = acc[C * i:C * i + C]

    def each(axis, turn, work):
        for step in (1, -1):
            pl.when(has[axis, turn * step])(lambda step=step: work(step))

    def start_faces(q, f, eb, half, parts=(0, 4)):
        def go(step):
            for k in parts:
                xcopy(q, f, eb, step, half, k).start()
        each("x", 1, go)

    def start_sides(q, f, eb, yb, planes):
        def rows(step):
            for p in planes:
                yrows(q, f, step, p).start()
        each("y", 1, rows)
        pack_edges(f, eb, planes)
        for p in planes:
            zcopy(q, eb, p).start()
        def strips_out(step):
            for p in planes:
                for other in range(2):
                    yedges(q, eb, yb, step, other, p).start()
        each("y", 1, strips_out)

    def pass_on(q, f, eb, yb, planes, half):
        def rows_in(step):
            for p in planes:
                yrows(q, f, step, p).wait_recv()
        each("y", -1, rows_in)
        def rows_on(step):
            xcopy(q, f, eb, step, half, 1).start()
            xcopy(q, f, eb, step, half, 2).start()
        each("x", 1, rows_on)
        for p in planes:
            zcopy(q, eb, p).wait_recv()
            zcopy(q, eb, p).wait_send()
        def strips_in(step):
            for p in planes:
                for other in range(2):
                    yedges(q, eb, yb, step, other, p).wait_recv()
        each("y", -1, strips_in)
        def strips_gone(step):
            for p in planes:
                for other in range(2):
                    yedges(q, eb, yb, step, other, p).wait_send()
        each("y", 1, strips_gone)
        low = lanes % 64
        for s in range(2):
            for p in planes:
                v = eb[s, p + 2]
                v = jnp.where(low < 2, pltpu.roll(yb[0, s, p], L - NYL, 1), v)
                v = jnp.where((low >= NYL + 2) & (low < NYL + 4), pltpu.roll(yb[1, s, p], NYL, 1), v)
                eb[s, p + 2] = v
        each("x", 1, lambda step: xcopy(q, f, eb, step, half, 3).start())

    def arrive(q, f, eb, half, parts=range(5)):
        def come(step):
            for k in parts:
                xcopy(q, f, eb, step, half, k).wait_recv()
        each("x", -1, come)

    def drain(q, f, eb):
        def xgone(step):
            for half in range(2):
                for k in range(5):
                    xcopy(q, f, eb, step, half, k).wait_send()
        each("x", 1, xgone)
        def ygone(step):
            for p in range(NXL):
                yrows(q, f, step, p).wait_send()
        each("y", 1, ygone)

    def make_weights(sec):
        for lay in range(2):
            base[...] = jnp.zeros_like(base)
            for dz in range(3):
                for dx in range(3):
                    for dy in range(3):
                        p = 16 * (dx * 6 + dy)
                        base[dz, :, p:p + 16] = wall[sec, lay, dx * 9 + dy * 3 + dz].astype(F32)
            brow[0:1, 0:C] = ball[sec, lay:lay + 1, :].astype(F32)
            for xq in range(2):
                for yq in range(4):
                    rows = slice(16 * (4 * xq + yq), 16 * (4 * xq + yq) + 16)
                    for dz in range(3):
                        v = base[dz]
                        if 6 * xq + yq:
                            v = pltpu.roll(v, 16 * (6 * xq + yq), 1)
                        tm[2 * sec + lay, rows, 384 * dz:384 * dz + 384] = v.astype(BF)
            br = jnp.broadcast_to(brow[0:1, :], (L, L))
            rr = lax.broadcasted_iota(jnp.int32, (L, L), 0)
            cc = lax.broadcasted_iota(jnp.int32, (L, L), 1)
            diag = jnp.where(rr % 16 == cc, br, 0.0).astype(BF)
            tm[2 * sec + lay, :, 1152:1280] = diag
            if lay == 0:
                wbase[...] = jnp.zeros_like(wbase)
                for dy in range(3):
                    for dx in range(3):
                        for col in range(3):
                            p = 16 * (dx * 3 + col)
                            dz = jnp.where(gz == 0, col, 2 - col)
                            wbase[16 * dy:16 * dy + 16, p:p + 16] = wall[
                                sec, 0, dx * 9 + dy * 3 + dz].astype(F32)
                wbase[16:32, 144:160] = diag[0:16, 0:16].astype(F32)
                ws[sec] = wbase[...].astype(BF)

    def shifted(v, n, lane):
        h = jnp.where(lanes == edge, pltpu.roll(n, (L - lane) % L, 1) if lane else n, zrow)
        return (jnp.where(lanes == 0, h, pltpu.roll(v, 1, 1)),
                jnp.where(lanes == L - 1, h, pltpu.roll(v, L - 1, 1)))

    def shift(f, eb, planes, first=0, last=NYL + 4):
        for x in planes:
            n = pltpu.roll(eb[1, x], edge, 1)
            for y in range(first, last):
                fm[x, y], fp[x, y] = shifted(f[x, y], n, y)

    def strips(sec, eb, todo):
        one = ones[0:C, :]
        tail = jnp.zeros((256 - 160, L), BF)
        lane = lax.broadcasted_iota(jnp.int32, (C, L), 1)
        for j in todo:
            rows = []
            for dx in range(3):
                rows += [eb[0, j + dx], eb[1, j + dx], pltpu.roll(eb[1, j + dx], 64, 1)]
            m = dots(ws[sec], jnp.concatenate(rows + [one, tail], axis=0))
            v = pltpu.roll(m[0:16], 1, 1) + m[16:32] + pltpu.roll(m[32:48], L - 1, 1)
            v = leaky(v)
            bad = (lane == 1) & (gy == 0) | (lane == NYL + 2) & (gy == ngy - 1)
            if j == 0:
                bad = bad | (gx == 0)
            if j == HX - 1:
                bad = bad | (gx == ngx - 1)
            hn[j] = jnp.where(bad, 0.0, v).astype(BF)

    def boxes(lay, fields, pairs, xqs):
        acc = None
        for k in range(5):
            cols = []
            for x0, y0 in pairs:
                rows = []
                for p in range(16 * k, min(16 * k + 16, 72)):
                    g, yr = divmod(p, 6)
                    rows.append(fields[g // 4][x0 + g % 4, y0 + yr])
                if k == 4:
                    rows.append(ones[...])
                cols.append(jnp.concatenate(rows, axis=0))
            t = dots(tm[lay, 64 * xqs[0]:64 * xqs[-1] + 64, 256 * k:256 * k + 256], jnp.concatenate(cols, axis=1))
            acc = t if acc is None else acc + t
        return leaky(acc).astype(BF)

    def layer(lay, fields, todo, xqs, put):
        for h in range(0, len(todo), 2):
            pairs = todo[h:h + 2]
            v = boxes(lay, fields, pairs, xqs)
            for k, (x0, y0) in enumerate(pairs):
                b = v[:, L * k:L * k + L].reshape(len(xqs), 4, C, L)
                for i, xq in enumerate(xqs):
                    for yq in range(4):
                        put(x0 + xq, y0 + yq, b[i, yq])

    def layer_a(sec, f, todo, xqs=(0, 1)):
        xs = sorted({x0 + xq for x0, _ in todo for xq in xqs})
        ns = {x: pltpu.roll(hn[x], edge, 1) for x in xs}
        def put(x, y, t):
            h0[x, y] = t
            hm[x, y], hp[x, y] = shifted(t, ns[x], y + 1)
        layer(2 * sec, (fm, f, fp), todo, xqs, put)

    def outside():
        for r in (h0, hm, hp):
            pl.when(gx == 0)(lambda r=r: clear(r, 0, 1, 0, HY))
            pl.when(gx == ngx - 1)(lambda r=r: clear(r, HX - 1, HX, 0, HY))
            pl.when(gy == 0)(lambda r=r: clear(r, 0, HX, 0, 1))
            pl.when(gy == ngy - 1)(lambda r=r: clear(r, 0, HX, NYL + 1, NYL + 2))

    def layer_b(sec, g, o, todo, xqs=(0, 1)):
        def put(x, y, t):
            g[o + x, o + y] = t
        layer(2 * sec + 1, (hm, h0, hp), todo, xqs, put)

    def send_out(q, g, o, x, y):
        ab = [g[o + x + k, pl.ds(o + y, 16)].reshape(256, L) for k in range(2)]
        t = dots(pm[...], jnp.concatenate(ab, axis=1)).astype(BF)
        for k in range(2):
            stage[q, :, x + k, y:y + 16, :] = t[:, L * k:L * k + L].reshape(C, 16, L)
        pl.when(seg == q)(lambda: lcopy(q, x, y).start())
        pl.when(seg != q)(lambda: ocopy(q, x, y).start())

    def boxes_of(xs, ny, first=0):
        return [(x, y) for y in range(first, ny, 4) for x in xs]

    near, far = (0, 3), (1, 2)
    start_faces(0, f1, eb1, 0)
    start_sides(0, f1, eb1, yb1, (0, 1, 2, 3))
    wl.wait()
    bl.wait()
    wcopy(0, wall).start()
    wcopy(1, ball).start()
    pass_on(0, f1, eb1, yb1, near, 0)
    pass_on(0, f1, eb1, yb1, far, 1)
    start_faces(0, f1, eb1, 1)
    brow[...] = jnp.zeros_like(brow)
    wcopy(0, wall, 1 - seg).wait_recv()
    wcopy(1, ball, 1 - seg).wait_recv()
    wcopy(0, wall).wait_send()
    wcopy(1, ball).wait_send()
    for f in (f1, f2, fm, fp):
        clear(f, 0, FX, NYL + 4, FY)
    for sec in range(2):
        make_weights(sec)

    arrive(0, f1, eb1, 0)
    shift(f1, eb1, range(1, FX - 1))
    strips(0, eb1, range(1, HX - 1))
    layer_a(0, f1, boxes_of((1, 3), HY))
    outside()
    layer_b(0, f2, 2, boxes_of((1,), NYL))
    start_faces(1, f2, eb2, 1)
    start_sides(1, f2, eb2, yb2, far)
    for part, (y0, y1, y2) in enumerate(((0, 20, 16), (20, HY, NYL))):
        arrive(0, f1, eb1, 1, ((0, 1, 3), (2, 4))[part])
        shift(f1, eb1, (0, FX - 1), (0, CUT[0] + 2)[part], (CUT[0] + 2, NYL + 4)[part])
        if part == 0:
            strips(0, eb1, (0, HX - 1))
        layer_a(0, f1, boxes_of((0,), y1, y0), (0,))
        layer_a(0, f1, boxes_of((4,), y1, y0), (1,))
        outside()
        layer_b(0, f2, 2, boxes_of((0,), y2, 16 * part), (0,))
        layer_b(0, f2, 2, boxes_of((2,), y2, 16 * part), (1,))
        start_faces(1, f2, eb2, 0, (4 * part,))

    start_sides(1, f2, eb2, yb2, near)
    for y in (0, 16):
        for x in (0, 2):
            send_out(0, f2, 2, x, y)
    pass_on(1, f2, eb2, yb2, far, 1)
    pass_on(1, f2, eb2, yb2, near, 0)
    shift(f2, eb2, range(2, FX - 2))
    strips(1, eb2, (2, 3))
    layer_a(1, f2, boxes_of((2,), HY))
    arrive(1, f2, eb2, 1)
    shift(f2, eb2, (0, FX - 1))
    arrive(1, f2, eb2, 0)
    shift(f2, eb2, (1, FX - 2))
    strips(1, eb2, (0, 1, 4, 5))
    layer_a(1, f2, boxes_of((0, 4), HY))
    outside()
    for y in (0, 16):
        for x in (0, 2):
            layer_b(1, res, 0, boxes_of((x,), y + 16, y))
            send_out(1, res, 0, x, y)
    drain(0, f1, eb1)
    drain(1, f2, eb2)

    for q in range(2):
        for y in (0, 16):
            for x in (0, 2):
                @pl.when(seg == q)
                def _(q=q, x=x, y=y):
                    lcopy(q, x, y).wait()
                    ocopy(q, x, y, 1 - seg).wait_recv()
                @pl.when(seg != q)
                def _(q=q, x=x, y=y):
                    ocopy(q, x, y).wait_send()


def shards(sizes, features, weights, biases):
    w = weights[0].transpose(0, 3, 4, 5, 1, 2).reshape(2, 27, C, C)
    hbm = pl.BlockSpec(memory_space=pltpu.HBM)
    dma = pltpu.SemaphoreType.DMA
    out = pl.pallas_call(
        functools.partial(kernel, sizes),
        name="sections",
        out_shape=jax.ShapeDtypeStruct((2, C, NXL, NYL, L), BF),
        in_specs=[hbm] * 3,
        out_specs=pl.BlockSpec(memory_space=pltpu.VMEM),
        scratch_shapes=[
            pltpu.VMEM((C, NXL, NYL, L), BF),
            pltpu.VMEM((2, 2, 27, C, C), BF),
            pltpu.VMEM((2, 2, C), BF),
            pltpu.VMEM((FX, FY, C, L), BF),
            pltpu.VMEM((FX, FY, C, L), BF),
            pltpu.VMEM((FX, FY, C, L), BF),
            pltpu.VMEM((FX, FY, C, L), BF),
            pltpu.VMEM((HX, HY, C, L), BF),
            pltpu.VMEM((HX, HY, C, L), BF),
            pltpu.VMEM((HX, HY, C, L), BF),
            pltpu.VMEM((4, L, KT), BF),
            pltpu.VMEM((2, 48, 256), BF),
            pltpu.VMEM((3, C, 384), F32),
            pltpu.VMEM((8, L), F32),
            pltpu.VMEM((48, 256), F32),
            pltpu.VMEM((256, 256), BF),
            pltpu.VMEM((L, L), BF),
            pltpu.VMEM((NYL * L, L), BF),
            pltpu.VMEM((2, FX, C, L), BF),
            pltpu.VMEM((2, FX, C, L), BF),
            pltpu.VMEM((2, 2, NXL, C, L), BF),
            pltpu.VMEM((2, 2, NXL, C, L), BF),
            pltpu.VMEM((HX, C, L), BF),
            pltpu.VMEM((NXL, NYL, C, L), BF),
            pltpu.VMEM((2, C, NXL, NYL, L), BF),
            dma((3,)), dma((2,)), dma((2,)),
            dma((2, 2, 2, 5)), dma((2, 2, 2, 5)),
            dma((2, 2, NXL)), dma((2, 2, NXL)),
            dma((2, 2, 2, NXL)), dma((2, 2, 2, NXL)),
            dma((2, NXL)), dma((2, NXL)), dma((2, 4)), dma((2, 4)), dma((2, 4)),
        ],
        compiler_params=pltpu.CompilerParams(
            collective_id=0, has_side_effects=True, vmem_limit_bytes=32 << 20),
    )(*(pltpu.with_memory_space_constraint(a, pltpu.HBM) for a in (features, w, biases[0])))
    return out[None]


def solution(mesh):
    placed = (
        P(None, None, "gx", "gy", "gz"),
        P("segment", None, None, None, None, None, None),
        P("segment", None, None),
    )
    sizes = (mesh.shape["gx"], mesh.shape["gy"])
    return jax.shard_map(
        functools.partial(shards, sizes),
        mesh=mesh,
        in_specs=placed,
        out_specs=P("segment", None, None, "gx", "gy", "gz"),
        check_vma=False,
    )
```

```python
import functools

import jax
import jax.numpy as jnp
from jax import lax
from jax.experimental import pallas as pl
from jax.experimental.pallas import tpu as pltpu
from jax.sharding import PartitionSpec as P

MESH = pl.DeviceIdType.MESH
BF = jnp.bfloat16
F32 = jnp.float32

NXL, NYL, C, L = 4, 32, 16, 128
FX, FY = NXL + 4, NYL + 6
HX, HY = NXL + 2, NYL + 4
CUT = (20, 16)
KT = 1280


def dots(a, b):
    return jnp.dot(a, b, preferred_element_type=F32)


def iota(shape, dim):
    return lax.broadcasted_iota(jnp.int32, shape, dim)


def one_hot(hit):
    return jnp.where(hit, 1.0, 0.0).astype(BF)


def leaky(v):
    return jnp.maximum(v, 0.2 * v)


def kernel(
    sizes, feat, wts, bias, out,
    raw, wall, ball, f1, f2, fm, fp, h0, hm, hp, tm, ws, base, brow, wbase, pm, ones, xe,
    eb1, eb2, yb1, yb2, hn, res, stage,
    lsem, wsem, wrs, ssx, rsx, ssy, rsy, sse, rse, ssz, rsz, sso, rso, osem,
):
    ngx, ngy = sizes
    seg, gx = lax.axis_index("segment"), lax.axis_index("gx")
    gy, gz = lax.axis_index("gy"), lax.axis_index("gz")
    has = {
        ("x", 1): gx < ngx - 1, ("x", -1): gx > 0,
        ("y", 1): gy < ngy - 1, ("y", -1): gy > 0,
    }
    here = {"x": gx, "y": gy}

    def to(axis, step):
        return {"g" + axis: here[axis] + step}

    lanes = iota((C, L), 1)
    edge = jnp.where(gz == 0, L - 1, 0)
    inner = jnp.where(gz == 0, L - 2, 1)

    load = pltpu.make_async_copy(feat.at[seg], raw, lsem.at[0])
    load.start()
    wl = pltpu.make_async_copy(wts, wall.at[seg], lsem.at[1])
    wl.start()
    bl = pltpu.make_async_copy(bias, ball.at[seg], lsem.at[2])
    bl.start()

    zrow = jnp.zeros((C, L), BF)

    def clear(ref, x0, x1, y0, y1):
        def body(i, c):
            for y in range(y0, y1):
                ref[i, y] = zrow
            return c
        lax.fori_loop(x0, x1, body, 0)

    def clear_strips(eb, yb, planes, d):
        for p in planes:
            eb[0, p] = zrow
            eb[1, p] = zrow
        if d is not None:
            for p in range(NXL):
                yb[d, 0, p] = zrow
                yb[d, 1, p] = zrow

    for f, eb, yb in ((f1, eb1, yb1), (f2, eb2, yb2)):
        @pl.when(gx == 0)
        def _(f=f, eb=eb, yb=yb):
            clear(f, 0, 2, 0, NYL + 4)
            clear_strips(eb, yb, (0, 1), None)
        @pl.when(gx == ngx - 1)
        def _(f=f, eb=eb, yb=yb):
            clear(f, FX - 2, FX, 0, NYL + 4)
            clear_strips(eb, yb, (FX - 2, FX - 1), None)
        @pl.when(gy == 0)
        def _(f=f, eb=eb, yb=yb):
            clear(f, 0, FX, 0, 2)
            clear_strips(eb, yb, (), 0)
        @pl.when(gy == ngy - 1)
        def _(f=f, eb=eb, yb=yb):
            clear(f, 0, FX, NYL + 2, NYL + 4)
            clear_strips(eb, yb, (), 1)

    bar = pltpu.get_barrier_semaphore()
    for (axis, step), ok in has.items():
        @pl.when(ok)
        def _(axis=axis, step=step):
            pl.semaphore_signal(bar, inc=1, device_id=to(axis, step), device_id_type=MESH)
            if axis == "y":
                pl.semaphore_signal(
                    bar, inc=1, device_id={"gy": gy + step, "gz": 1 - gz}, device_id_type=MESH)
    pl.semaphore_signal(bar, inc=1, device_id={"gz": 1 - gz}, device_id_type=MESH)
    pl.semaphore_signal(bar, inc=1, device_id={"segment": 1 - seg}, device_id_type=MESH)

    r = lax.broadcasted_iota(jnp.int32, (256, 256), 0)
    c = lax.broadcasted_iota(jnp.int32, (256, 256), 1)
    pm[...] = jnp.where((r // 16 == c % 16) & (r % 16 == c // 16), 1.0, 0.0).astype(BF)
    orow = lax.broadcasted_iota(jnp.int32, (L, L), 0)
    ones[...] = jnp.where(orow < C, 1.0, 0.0).astype(BF)
    re, ce = iota((L, L), 0), iota((L, L), 1)
    def table_e(y, carry):
        hit = (re == edge) & (ce == y + 2) | (re == inner) & (ce == y + 66)
        xe[pl.ds(pl.multiple_of(L * y, L), L), :] = one_hot(hit)
        return carry
    lax.fori_loop(0, NYL, table_e, 0)
    load.wait()
    for y in range(NYL // 16):
        for x in range(0, NXL, 2):
            ab = [raw[:, x + k, 16 * y:16 * y + 16, :].reshape(256, L) for k in range(2)]
            t = dots(pm[...], jnp.concatenate(ab, axis=1)).astype(BF)
            for k in range(2):
                f1[x + k + 2, pl.ds(2 + 16 * y, 16)] = t[:, L * k:L * k + L].reshape(16, C, L)

    count = 2 + sum(
        jnp.where(ok, 2 if axis == "y" else 1, 0) for (axis, _), ok in has.items())
    pl.semaphore_wait(bar, count)

    def xcopy(q, f, eb, step, half, k):
        d = 0 if step > 0 else 1
        mv = -NXL * step
        src = (FX - 3, FX - 4)[half] if step > 0 else (2, 3)[half]
        part = (
            lambda x: f.at[x, pl.ds(2, CUT[q])],
            lambda x: f.at[x, pl.ds(0, 2)],
            lambda x: f.at[x, pl.ds(NYL + 2, 2)],
            lambda x: eb.at[:, x],
            lambda x: f.at[x, pl.ds(2 + CUT[q], NYL - CUT[q])],
        )[k]
        return pltpu.make_async_remote_copy(
            part(src), part(src + mv), ssx.at[q, d, half, k], rsx.at[q, d, half, k],
            device_id=to("x", step), device_id_type=MESH)

    def yrows(q, f, step, p):
        d = 0 if step > 0 else 1
        src, dst = (NYL, 0) if step > 0 else (2, NYL + 2)
        return pltpu.make_async_remote_copy(
            f.at[2 + p, pl.ds(src, 2)], f.at[2 + p, pl.ds(dst, 2)],
            ssy.at[q, d, p], rsy.at[q, d, p], device_id=to("y", step), device_id_type=MESH)

    def yedges(q, eb, yb, step, other, p):
        d = 0 if step > 0 else 1
        return pltpu.make_async_remote_copy(
            eb.at[0, 2 + p], yb.at[d, other, p],
            sse.at[q, d, other, p], rse.at[q, d, other, p],
            device_id={"gy": gy + step, "gz": 1 - gz if other else gz}, device_id_type=MESH)

    def zcopy(q, eb, p):
        return pltpu.make_async_remote_copy(
            eb.at[0, 2 + p], eb.at[1, 2 + p], ssz.at[q, p], rsz.at[q, p],
            device_id={"gz": 1 - gz}, device_id_type=MESH)

    def piece(ref, x, y):
        return ref.at[:, pl.ds(x, 2), pl.ds(y, 16)]

    def ocopy(q, x, y, slot=seg):
        n = x // 2 + y // 8
        return pltpu.make_async_remote_copy(
            piece(stage.at[q], x, y), piece(out.at[slot], x, y), sso.at[q, n], rso.at[q, n],
            device_id={"segment": 1 - seg}, device_id_type=MESH)

    def lcopy(q, x, y):
        return pltpu.make_async_copy(
            piece(stage.at[q], x, y), piece(out.at[seg], x, y), osem.at[q, x // 2 + y // 8])

    def wcopy(k, ref, sec=seg):
        return pltpu.make_async_remote_copy(
            ref.at[sec], ref.at[sec], wsem.at[k], wrs.at[k],
            device_id={"segment": 1 - seg}, device_id_type=MESH)


    def pack_edges(f, eb, planes):
        acc = None
        for y in range(0, NYL, 2):
            lhs = [jnp.concatenate([f[2 + p, 2 + y + k] for p in planes], axis=0) for k in range(2)]
            t = dots(jnp.concatenate(lhs, axis=1), xe[pl.ds(L * y, 2 * L), :])
            acc = t if acc is None else acc + t
        acc = acc.astype(BF)
        for i, p in enumerate(planes):
            eb[0, 2 + p] = acc[C * i:C * i + C]

    def each(axis, turn, work):
        for step in (1, -1):
            pl.when(has[axis, turn * step])(lambda step=step: work(step))

    def start_faces(q, f, eb, half, parts=(0, 4)):
        def go(step):
            for k in parts:
                xcopy(q, f, eb, step, half, k).start()
        each("x", 1, go)

    def start_sides(q, f, eb, yb, planes):
        def rows(step):
            for p in planes:
                yrows(q, f, step, p).start()
        each("y", 1, rows)
        pack_edges(f, eb, planes)
        for p in planes:
            zcopy(q, eb, p).start()
        def strips_out(step):
            for p in planes:
                for other in range(2):
                    yedges(q, eb, yb, step, other, p).start()
        each("y", 1, strips_out)

    def pass_on(q, f, eb, yb, planes, half):
        def rows_in(step):
            for p in planes:
                yrows(q, f, step, p).wait_recv()
        each("y", -1, rows_in)
        def rows_on(step):
            xcopy(q, f, eb, step, half, 1).start()
            xcopy(q, f, eb, step, half, 2).start()
        each("x", 1, rows_on)
        for p in planes:
            zcopy(q, eb, p).wait_recv()
            zcopy(q, eb, p).wait_send()
        def strips_in(step):
            for p in planes:
                for other in range(2):
                    yedges(q, eb, yb, step, other, p).wait_recv()
        each("y", -1, strips_in)
        def strips_gone(step):
            for p in planes:
                for other in range(2):
                    yedges(q, eb, yb, step, other, p).wait_send()
        each("y", 1, strips_gone)
        low = lanes % 64
        for s in range(2):
            for p in planes:
                v = eb[s, p + 2]
                v = jnp.where(low < 2, pltpu.roll(yb[0, s, p], L - NYL, 1), v)
                v = jnp.where((low >= NYL + 2) & (low < NYL + 4), pltpu.roll(yb[1, s, p], NYL, 1), v)
                eb[s, p + 2] = v
        each("x", 1, lambda step: xcopy(q, f, eb, step, half, 3).start())

    def arrive(q, f, eb, half, parts=range(5)):
        def come(step):
            for k in parts:
                xcopy(q, f, eb, step, half, k).wait_recv()
        each("x", -1, come)

    def drain(q, f, eb):
        def xgone(step):
            for half in range(2):
                for k in range(5):
                    xcopy(q, f, eb, step, half, k).wait_send()
        each("x", 1, xgone)
        def ygone(step):
            for p in range(NXL):
                yrows(q, f, step, p).wait_send()
        each("y", 1, ygone)

    def make_weights(sec):
        for lay in range(2):
            base[...] = jnp.zeros_like(base)
            for dz in range(3):
                for dx in range(3):
                    for dy in range(3):
                        p = 16 * (dx * 6 + dy)
                        base[dz, :, p:p + 16] = wall[sec, lay, dx * 9 + dy * 3 + dz].astype(F32)
            brow[0:1, 0:C] = ball[sec, lay:lay + 1, :].astype(F32)
            for xq in range(2):
                for yq in range(4):
                    rows = slice(16 * (4 * xq + yq), 16 * (4 * xq + yq) + 16)
                    for dz in range(3):
                        v = base[dz]
                        if 6 * xq + yq:
                            v = pltpu.roll(v, 16 * (6 * xq + yq), 1)
                        tm[2 * sec + lay, rows, 384 * dz:384 * dz + 384] = v.astype(BF)
            br = jnp.broadcast_to(brow[0:1, :], (L, L))
            rr = lax.broadcasted_iota(jnp.int32, (L, L), 0)
            cc = lax.broadcasted_iota(jnp.int32, (L, L), 1)
            diag = jnp.where(rr % 16 == cc, br, 0.0).astype(BF)
            tm[2 * sec + lay, :, 1152:1280] = diag
            if lay == 0:
                wbase[...] = jnp.zeros_like(wbase)
                for dy in range(3):
                    for dx in range(3):
                        for col in range(3):
                            p = 16 * (dx * 3 + col)
                            dz = jnp.where(gz == 0, col, 2 - col)
                            wbase[16 * dy:16 * dy + 16, p:p + 16] = wall[
                                sec, 0, dx * 9 + dy * 3 + dz].astype(F32)
                wbase[16:32, 144:160] = diag[0:16, 0:16].astype(F32)
                ws[sec] = wbase[...].astype(BF)

    def shifted(v, n, lane):
        h = jnp.where(lanes == edge, pltpu.roll(n, (L - lane) % L, 1) if lane else n, zrow)
        return (jnp.where(lanes == 0, h, pltpu.roll(v, 1, 1)),
                jnp.where(lanes == L - 1, h, pltpu.roll(v, L - 1, 1)))

    def shift(f, eb, planes, first=0, last=NYL + 4):
        for x in planes:
            n = pltpu.roll(eb[1, x], edge, 1)
            for y in range(first, last):
                fm[x, y], fp[x, y] = shifted(f[x, y], n, y)

    def strips(sec, eb, todo):
        one = ones[0:C, :]
        tail = jnp.zeros((256 - 160, L), BF)
        lane = lax.broadcasted_iota(jnp.int32, (C, L), 1)
        for j in todo:
            rows = []
            for dx in range(3):
                rows += [eb[0, j + dx], eb[1, j + dx], pltpu.roll(eb[1, j + dx], 64, 1)]
            m = dots(ws[sec], jnp.concatenate(rows + [one, tail], axis=0))
            v = pltpu.roll(m[0:16], 1, 1) + m[16:32] + pltpu.roll(m[32:48], L - 1, 1)
            v = leaky(v)
            bad = (lane == 1) & (gy == 0) | (lane == NYL + 2) & (gy == ngy - 1)
            bad = bad | (j == 0) & (gx == 0) | (j == HX - 1) & (gx == ngx - 1)
            hn[j] = jnp.where(bad, 0.0, v).astype(BF)

    def boxes(lay, fields, pairs, rows_of):
        acc = None
        for k in range(5):
            cols = []
            for x0, y0 in pairs:
                rows = []
                for p in range(16 * k, min(16 * k + 16, 72)):
                    g, yr = divmod(p, 6)
                    rows.append(fields[g // 4][x0 + g % 4, y0 + yr])
                if k == 4:
                    rows.append(ones[...])
                cols.append(jnp.concatenate(rows, axis=0))
            t = dots(tm[lay, rows_of, 256 * k:256 * k + 256], jnp.concatenate(cols, axis=1))
            acc = t if acc is None else acc + t
        return leaky(acc).astype(BF)

    def layer(lay, fields, todo, xqs, put):
        if len(xqs) == 2:
            rows_of = slice(0, L)
        else:
            rows_of = pl.ds(pl.multiple_of(64 * xqs[0], 64), 64)
        for h in range(0, len(todo), 2):
            pairs = todo[h:h + 2]
            v = boxes(lay, fields, pairs, rows_of)
            for k, (x0, y0) in enumerate(pairs):
                b = v[:, L * k:L * k + L].reshape(len(xqs), 4, C, L)
                for i in range(len(xqs)):
                    for yq in range(4):
                        put(x0, i, y0 + yq, b[i, yq])

    def layer_a(sec, f, todo, xqs=(0, 1)):
        ns = {}
        for x0, _ in todo:
            for i, xq in enumerate(xqs):
                if (id(x0), i) not in ns:
                    ns[id(x0), i] = pltpu.roll(hn[x0 + xq], edge, 1)
        def put(x0, i, y, t):
            x = x0 + xqs[i]
            h0[x, y] = t
            hm[x, y], hp[x, y] = shifted(t, ns[id(x0), i], y + 1)
        layer(2 * sec, (fm, f, fp), todo, xqs, put)

    def outside():
        for r in (h0, hm, hp):
            pl.when(gx == 0)(lambda r=r: clear(r, 0, 1, 0, HY))
            pl.when(gx == ngx - 1)(lambda r=r: clear(r, HX - 1, HX, 0, HY))
            pl.when(gy == 0)(lambda r=r: clear(r, 0, HX, 0, 1))
            pl.when(gy == ngy - 1)(lambda r=r: clear(r, 0, HX, NYL + 1, NYL + 2))

    def layer_b(sec, g, o, todo, xqs=(0, 1)):
        def put(x0, i, y, t):
            g[o + x0 + xqs[i], o + y] = t
        layer(2 * sec + 1, (hm, h0, hp), todo, xqs, put)

    def send_out(q, g, o, x, y):
        ab = [g[o + x + k, pl.ds(o + y, 16)].reshape(256, L) for k in range(2)]
        t = dots(pm[...], jnp.concatenate(ab, axis=1)).astype(BF)
        for k in range(2):
            stage[q, :, x + k, y:y + 16, :] = t[:, L * k:L * k + L].reshape(C, 16, L)
        pl.when(seg == q)(lambda: lcopy(q, x, y).start())
        pl.when(seg != q)(lambda: ocopy(q, x, y).start())

    def boxes_of(xs, ny, first=0):
        return [(x, y) for y in range(first, ny, 4) for x in xs]

    near, far = (0, 3), (1, 2)
    start_faces(0, f1, eb1, 0)
    start_sides(0, f1, eb1, yb1, (0, 1, 2, 3))
    wl.wait()
    bl.wait()
    wcopy(0, wall).start()
    wcopy(1, ball).start()
    pass_on(0, f1, eb1, yb1, near, 0)
    start_faces(0, f1, eb1, 1)
    pass_on(0, f1, eb1, yb1, far, 1)
    brow[...] = jnp.zeros_like(brow)
    wcopy(0, wall, 1 - seg).wait_recv()
    wcopy(1, ball, 1 - seg).wait_recv()
    wcopy(0, wall).wait_send()
    wcopy(1, ball).wait_send()
    for f in (f1, f2, fm, fp):
        clear(f, 0, FX, NYL + 4, FY)
    for sec in range(2):
        make_weights(sec)

    arrive(0, f1, eb1, 0)
    shift(f1, eb1, range(1, FX - 1))
    strips(0, eb1, range(1, HX - 1))
    layer_a(0, f1, boxes_of((1, 3), HY))
    outside()
    layer_b(0, f2, 2, boxes_of((1,), NYL))
    start_faces(1, f2, eb2, 1)
    start_sides(1, f2, eb2, yb2, far)
    def on_side(side, work):
        for step in (1, -1):
            mine = side == (0 if step > 0 else 1)
            pl.when(mine & has["x", -step])(lambda step=step: work(step))

    def arrive_side(q, f, eb, half, side):
        def come(step):
            for k in range(5):
                xcopy(q, f, eb, step, half, k).wait_recv()
        on_side(side, come)

    def late(i, carry):
        side = jnp.where(gx < ngx // 2, i, 1 - i)
        arrive_side(0, f1, eb1, 1, side)
        shift(f1, eb1, ((FX - 1) * side,))
        strips(0, eb1, ((HX - 1) * side,))
        x0 = 4 * side
        layer_a(0, f1, [(x0, y) for y in range(0, HY, 4)], (side,))
        outside()
        x1 = 2 * side
        layer_b(0, f2, 2, [(x1, y) for y in range(0, NYL, 4)], (side,))
        def go(step):
            xcopy(1, f2, eb2, -step, 0, 0).start()
            xcopy(1, f2, eb2, -step, 0, 4).start()
        on_side(side, go)
        return carry
    lax.fori_loop(0, 2, late, 0)

    start_sides(1, f2, eb2, yb2, near)
    for y in (0, 16):
        for x in (0, 2):
            send_out(0, f2, 2, x, y)
    pass_on(1, f2, eb2, yb2, far, 1)
    pass_on(1, f2, eb2, yb2, near, 0)
    shift(f2, eb2, range(2, FX - 2))
    strips(1, eb2, (2, 3))
    layer_a(1, f2, boxes_of((2,), HY))
    def last(i, carry):
        side = jnp.where(gx < ngx // 2, i, 1 - i)
        arrive_side(1, f2, eb2, 1, side)
        shift(f2, eb2, ((FX - 1) * side,))
        arrive_side(1, f2, eb2, 0, side)
        shift(f2, eb2, (1 + (FX - 3) * side,))
        strips(1, eb2, (4 * side, 4 * side + 1))
        x0 = 4 * side
        layer_a(1, f2, [(x0, y) for y in range(0, HY, 4)])
        outside()
        x1 = 2 * side
        layer_b(1, res, 0, [(x1, y) for y in range(0, NYL, 4)])
        for y in (0, 16):
            send_out(1, res, 0, x1, y)
        return carry
    lax.fori_loop(0, 2, last, 0)
    drain(0, f1, eb1)
    drain(1, f2, eb2)

    for q in range(2):
        for y in (0, 16):
            for x in (0, 2):
                @pl.when(seg == q)
                def _(q=q, x=x, y=y):
                    lcopy(q, x, y).wait()
                    ocopy(q, x, y, 1 - seg).wait_recv()
                @pl.when(seg != q)
                def _(q=q, x=x, y=y):
                    ocopy(q, x, y).wait_send()


def shards(sizes, features, weights, biases):
    w = weights[0].transpose(0, 3, 4, 5, 1, 2).reshape(2, 27, C, C)
    hbm = pl.BlockSpec(memory_space=pltpu.HBM)
    dma = pltpu.SemaphoreType.DMA
    out = pl.pallas_call(
        functools.partial(kernel, sizes),
        name="sections",
        out_shape=jax.ShapeDtypeStruct((2, C, NXL, NYL, L), BF),
        in_specs=[hbm] * 3,
        out_specs=pl.BlockSpec(memory_space=pltpu.VMEM),
        scratch_shapes=[
            pltpu.VMEM((C, NXL, NYL, L), BF),
            pltpu.VMEM((2, 2, 27, C, C), BF),
            pltpu.VMEM((2, 2, C), BF),
            pltpu.VMEM((FX, FY, C, L), BF),
            pltpu.VMEM((FX, FY, C, L), BF),
            pltpu.VMEM((FX, FY, C, L), BF),
            pltpu.VMEM((FX, FY, C, L), BF),
            pltpu.VMEM((HX, HY, C, L), BF),
            pltpu.VMEM((HX, HY, C, L), BF),
            pltpu.VMEM((HX, HY, C, L), BF),
            pltpu.VMEM((4, L, KT), BF),
            pltpu.VMEM((2, 48, 256), BF),
            pltpu.VMEM((3, C, 384), F32),
            pltpu.VMEM((8, L), F32),
            pltpu.VMEM((48, 256), F32),
            pltpu.VMEM((256, 256), BF),
            pltpu.VMEM((L, L), BF),
            pltpu.VMEM((NYL * L, L), BF),
            pltpu.VMEM((2, FX, C, L), BF),
            pltpu.VMEM((2, FX, C, L), BF),
            pltpu.VMEM((2, 2, NXL, C, L), BF),
            pltpu.VMEM((2, 2, NXL, C, L), BF),
            pltpu.VMEM((HX, C, L), BF),
            pltpu.VMEM((NXL, NYL, C, L), BF),
            pltpu.VMEM((2, C, NXL, NYL, L), BF),
            dma((3,)), dma((2,)), dma((2,)),
            dma((2, 2, 2, 5)), dma((2, 2, 2, 5)),
            dma((2, 2, NXL)), dma((2, 2, NXL)),
            dma((2, 2, 2, NXL)), dma((2, 2, 2, NXL)),
            dma((2, NXL)), dma((2, NXL)), dma((2, 4)), dma((2, 4)), dma((2, 4)),
        ],
        compiler_params=pltpu.CompilerParams(
            collective_id=0, has_side_effects=True, vmem_limit_bytes=32 << 20),
    )(*(pltpu.with_memory_space_constraint(a, pltpu.HBM) for a in (features, w, biases[0])))
    return out[None]


def solution(mesh):
    placed = (
        P(None, None, "gx", "gy", "gz"),
        P("segment", None, None, None, None, None, None),
        P("segment", None, None),
    )
    sizes = (mesh.shape["gx"], mesh.shape["gy"])
    return jax.shard_map(
        functools.partial(shards, sizes),
        mesh=mesh,
        in_specs=placed,
        out_specs=P("segment", None, None, "gx", "gy", "gz"),
        check_vma=False,
    )
```

```python
import functools

import jax
import jax.numpy as jnp
from jax import lax
from jax.experimental import pallas as pl
from jax.experimental.pallas import tpu as pltpu
from jax.sharding import PartitionSpec as P

MESH = pl.DeviceIdType.MESH
BF = jnp.bfloat16
F32 = jnp.float32

NXL, NYL, C, L = 4, 32, 16, 128
FX, FY = NXL + 4, NYL + 6
HX, HY = NXL + 2, NYL + 4
CUT = (20, 16)
KT = 1280


def dots(a, b):
    return jnp.dot(a, b, preferred_element_type=F32)


def iota(shape, dim):
    return lax.broadcasted_iota(jnp.int32, shape, dim)


def one_hot(hit):
    return jnp.where(hit, 1.0, 0.0).astype(BF)


def leaky(v):
    return jnp.maximum(v, 0.2 * v)


def kernel(
    sizes, feat, wts, bias, out,
    raw, wall, ball, f1, f2, fm, fp, h0, hm, hp, tm, ws, base, brow, wbase, pm, ones, xe,
    eb1, eb2, yb1, yb2, hn, res, stage,
    lsem, wsem, wrs, ssx, rsx, ssy, rsy, sse, rse, ssz, rsz, sso, rso, osem,
):
    ngx, ngy = sizes
    seg, gx = lax.axis_index("segment"), lax.axis_index("gx")
    gy, gz = lax.axis_index("gy"), lax.axis_index("gz")
    has = {
        ("x", 1): gx < ngx - 1, ("x", -1): gx > 0,
        ("y", 1): gy < ngy - 1, ("y", -1): gy > 0,
    }
    here = {"x": gx, "y": gy}

    def to(axis, step):
        return {"g" + axis: here[axis] + step}

    lanes = iota((C, L), 1)
    edge = jnp.where(gz == 0, L - 1, 0)
    inner = jnp.where(gz == 0, L - 2, 1)

    load = pltpu.make_async_copy(feat.at[seg], raw, lsem.at[0])
    load.start()
    wl = pltpu.make_async_copy(wts, wall.at[seg], lsem.at[1])
    wl.start()
    bl = pltpu.make_async_copy(bias, ball.at[seg], lsem.at[2])
    bl.start()

    zrow = jnp.zeros((C, L), BF)

    def clear(ref, x0, x1, y0, y1):
        def body(i, c):
            for y in range(y0, y1):
                ref[i, y] = zrow
            return c
        lax.fori_loop(x0, x1, body, 0)

    def clear_strips(eb, yb, planes, d):
        for p in planes:
            eb[0, p] = zrow
            eb[1, p] = zrow
        if d is not None:
            for p in range(NXL):
                yb[d, 0, p] = zrow
                yb[d, 1, p] = zrow

    for f, eb, yb in ((f1, eb1, yb1), (f2, eb2, yb2)):
        @pl.when(gx == 0)
        def _(f=f, eb=eb, yb=yb):
            clear(f, 0, 2, 0, NYL + 4)
            clear_strips(eb, yb, (0, 1), None)
        @pl.when(gx == ngx - 1)
        def _(f=f, eb=eb, yb=yb):
            clear(f, FX - 2, FX, 0, NYL + 4)
            clear_strips(eb, yb, (FX - 2, FX - 1), None)
        @pl.when(gy == 0)
        def _(f=f, eb=eb, yb=yb):
            clear(f, 0, FX, 0, 2)
            clear_strips(eb, yb, (), 0)
        @pl.when(gy == ngy - 1)
        def _(f=f, eb=eb, yb=yb):
            clear(f, 0, FX, NYL + 2, NYL + 4)
            clear_strips(eb, yb, (), 1)

    bar = pltpu.get_barrier_semaphore()
    for (axis, step), ok in has.items():
        @pl.when(ok)
        def _(axis=axis, step=step):
            pl.semaphore_signal(bar, inc=1, device_id=to(axis, step), device_id_type=MESH)
            if axis == "y":
                pl.semaphore_signal(
                    bar, inc=1, device_id={"gy": gy + step, "gz": 1 - gz}, device_id_type=MESH)
    pl.semaphore_signal(bar, inc=1, device_id={"gz": 1 - gz}, device_id_type=MESH)
    pl.semaphore_signal(bar, inc=1, device_id={"segment": 1 - seg}, device_id_type=MESH)

    r = lax.broadcasted_iota(jnp.int32, (256, 256), 0)
    c = lax.broadcasted_iota(jnp.int32, (256, 256), 1)
    pm[...] = jnp.where((r // 16 == c % 16) & (r % 16 == c // 16), 1.0, 0.0).astype(BF)
    orow = lax.broadcasted_iota(jnp.int32, (L, L), 0)
    ones[...] = jnp.where(orow < C, 1.0, 0.0).astype(BF)
    re, ce = iota((L, L), 0), iota((L, L), 1)
    def table_e(y, carry):
        hit = (re == edge) & (ce == y + 2) | (re == inner) & (ce == y + 66)
        xe[pl.ds(pl.multiple_of(L * y, L), L), :] = one_hot(hit)
        return carry
    lax.fori_loop(0, NYL, table_e, 0)
    load.wait()
    for y in range(NYL // 16):
        for x in range(0, NXL, 2):
            ab = [raw[:, x + k, 16 * y:16 * y + 16, :].reshape(256, L) for k in range(2)]
            t = dots(pm[...], jnp.concatenate(ab, axis=1)).astype(BF)
            for k in range(2):
                f1[x + k + 2, pl.ds(2 + 16 * y, 16)] = t[:, L * k:L * k + L].reshape(16, C, L)

    count = 2 + sum(
        jnp.where(ok, 2 if axis == "y" else 1, 0) for (axis, _), ok in has.items())
    pl.semaphore_wait(bar, count)

    def xcopy(q, f, eb, step, half, k):
        d = 0 if step > 0 else 1
        mv = -NXL * step
        src = (FX - 3, FX - 4)[half] if step > 0 else (2, 3)[half]
        part = (
            lambda x: f.at[x, pl.ds(2, CUT[q])],
            lambda x: f.at[x, pl.ds(0, 2)],
            lambda x: f.at[x, pl.ds(NYL + 2, 2)],
            lambda x: eb.at[:, x],
            lambda x: f.at[x, pl.ds(2 + CUT[q], NYL - CUT[q])],
        )[k]
        return pltpu.make_async_remote_copy(
            part(src), part(src + mv), ssx.at[q, d, half, k], rsx.at[q, d, half, k],
            device_id=to("x", step), device_id_type=MESH)

    def yrows(q, f, step, p):
        d = 0 if step > 0 else 1
        src, dst = (NYL, 0) if step > 0 else (2, NYL + 2)
        return pltpu.make_async_remote_copy(
            f.at[2 + p, pl.ds(src, 2)], f.at[2 + p, pl.ds(dst, 2)],
            ssy.at[q, d, p], rsy.at[q, d, p], device_id=to("y", step), device_id_type=MESH)

    def yedges(q, eb, yb, step, other, p):
        d = 0 if step > 0 else 1
        return pltpu.make_async_remote_copy(
            eb.at[0, 2 + p], yb.at[d, other, p],
            sse.at[q, d, other, p], rse.at[q, d, other, p],
            device_id={"gy": gy + step, "gz": 1 - gz if other else gz}, device_id_type=MESH)

    def zcopy(q, eb, p):
        return pltpu.make_async_remote_copy(
            eb.at[0, 2 + p], eb.at[1, 2 + p], ssz.at[q, p], rsz.at[q, p],
            device_id={"gz": 1 - gz}, device_id_type=MESH)

    def piece(ref, x, y):
        return ref.at[:, pl.ds(x, 2), pl.ds(y, 16)]

    def ocopy(q, x, y, slot=seg):
        n = x // 2 + y // 8
        return pltpu.make_async_remote_copy(
            piece(stage.at[q], x, y), piece(out.at[slot], x, y), sso.at[q, n], rso.at[q, n],
            device_id={"segment": 1 - seg}, device_id_type=MESH)

    def lcopy(q, x, y):
        return pltpu.make_async_copy(
            piece(stage.at[q], x, y), piece(out.at[seg], x, y), osem.at[q, x // 2 + y // 8])

    def wcopy(k, ref, sec=seg):
        return pltpu.make_async_remote_copy(
            ref.at[sec], ref.at[sec], wsem.at[k], wrs.at[k],
            device_id={"segment": 1 - seg}, device_id_type=MESH)


    def pack_edges(f, eb, planes):
        acc = None
        for y in range(0, NYL, 2):
            lhs = [jnp.concatenate([f[2 + p, 2 + y + k] for p in planes], axis=0) for k in range(2)]
            t = dots(jnp.concatenate(lhs, axis=1), xe[pl.ds(L * y, 2 * L), :])
            acc = t if acc is None else acc + t
        acc = acc.astype(BF)
        for i, p in enumerate(planes):
            eb[0, 2 + p] = acc[C * i:C * i + C]

    def each(axis, turn, work):
        for step in (1, -1):
            pl.when(has[axis, turn * step])(lambda step=step: work(step))

    def start_faces(q, f, eb, half, parts=(0, 4)):
        def go(step):
            for k in parts:
                xcopy(q, f, eb, step, half, k).start()
        each("x", 1, go)

    def start_sides(q, f, eb, yb, planes):
        def rows(step):
            for p in planes:
                yrows(q, f, step, p).start()
        each("y", 1, rows)
        pack_edges(f, eb, planes)
        for p in planes:
            zcopy(q, eb, p).start()
        def strips_out(step):
            for p in planes:
                for other in range(2):
                    yedges(q, eb, yb, step, other, p).start()
        each("y", 1, strips_out)

    def pass_on(q, f, eb, yb, planes, half):
        def rows_in(step):
            for p in planes:
                yrows(q, f, step, p).wait_recv()
        each("y", -1, rows_in)
        def rows_on(step):
            xcopy(q, f, eb, step, half, 1).start()
            xcopy(q, f, eb, step, half, 2).start()
        each("x", 1, rows_on)
        for p in planes:
            zcopy(q, eb, p).wait_recv()
            zcopy(q, eb, p).wait_send()
        def strips_in(step):
            for p in planes:
                for other in range(2):
                    yedges(q, eb, yb, step, other, p).wait_recv()
        each("y", -1, strips_in)
        def strips_gone(step):
            for p in planes:
                for other in range(2):
                    yedges(q, eb, yb, step, other, p).wait_send()
        each("y", 1, strips_gone)
        low = lanes % 64
        for s in range(2):
            for p in planes:
                v = eb[s, p + 2]
                v = jnp.where(low < 2, pltpu.roll(yb[0, s, p], L - NYL, 1), v)
                v = jnp.where((low >= NYL + 2) & (low < NYL + 4), pltpu.roll(yb[1, s, p], NYL, 1), v)
                eb[s, p + 2] = v
        each("x", 1, lambda step: xcopy(q, f, eb, step, half, 3).start())

    def arrive(q, f, eb, half, parts=range(5)):
        def come(step):
            for k in parts:
                xcopy(q, f, eb, step, half, k).wait_recv()
        each("x", -1, come)

    def drain(q, f, eb):
        def xgone(step):
            for half in range(2):
                for k in range(5):
                    xcopy(q, f, eb, step, half, k).wait_send()
        each("x", 1, xgone)
        def ygone(step):
            for p in range(NXL):
                yrows(q, f, step, p).wait_send()
        each("y", 1, ygone)

    def make_weights(sec):
        for lay in range(2):
            base[...] = jnp.zeros_like(base)
            for dz in range(3):
                for dx in range(3):
                    for dy in range(3):
                        p = 16 * (dx * 6 + dy)
                        base[dz, :, p:p + 16] = wall[sec, lay, dx * 9 + dy * 3 + dz].astype(F32)
            brow[0:1, 0:C] = ball[sec, lay:lay + 1, :].astype(F32)
            for xq in range(2):
                for yq in range(4):
                    rows = slice(16 * (4 * xq + yq), 16 * (4 * xq + yq) + 16)
                    for dz in range(3):
                        v = base[dz]
                        if 6 * xq + yq:
                            v = pltpu.roll(v, 16 * (6 * xq + yq), 1)
                        tm[2 * sec + lay, rows, 384 * dz:384 * dz + 384] = v.astype(BF)
            br = jnp.broadcast_to(brow[0:1, :], (L, L))
            rr = lax.broadcasted_iota(jnp.int32, (L, L), 0)
            cc = lax.broadcasted_iota(jnp.int32, (L, L), 1)
            diag = jnp.where(rr % 16 == cc, br, 0.0).astype(BF)
            tm[2 * sec + lay, :, 1152:1280] = diag
            if lay == 0:
                wbase[...] = jnp.zeros_like(wbase)
                for dy in range(3):
                    for dx in range(3):
                        for col in range(3):
                            p = 16 * (dx * 3 + col)
                            dz = jnp.where(gz == 0, col, 2 - col)
                            wbase[16 * dy:16 * dy + 16, p:p + 16] = wall[
                                sec, 0, dx * 9 + dy * 3 + dz].astype(F32)
                wbase[16:32, 144:160] = diag[0:16, 0:16].astype(F32)
                ws[sec] = wbase[...].astype(BF)

    def shifted(v, n, lane):
        h = jnp.where(lanes == edge, pltpu.roll(n, (L - lane) % L, 1) if lane else n, zrow)
        return (jnp.where(lanes == 0, h, pltpu.roll(v, 1, 1)),
                jnp.where(lanes == L - 1, h, pltpu.roll(v, L - 1, 1)))

    def shift(f, eb, planes, first=0, last=NYL + 4):
        for x in planes:
            n = pltpu.roll(eb[1, x], edge, 1)
            for y in range(first, last):
                fm[x, y], fp[x, y] = shifted(f[x, y], n, y)

    def strips(sec, eb, todo):
        one = ones[0:C, :]
        tail = jnp.zeros((256 - 160, L), BF)
        lane = lax.broadcasted_iota(jnp.int32, (C, L), 1)
        for j in todo:
            rows = []
            for dx in range(3):
                rows += [eb[0, j + dx], eb[1, j + dx], pltpu.roll(eb[1, j + dx], 64, 1)]
            m = dots(ws[sec], jnp.concatenate(rows + [one, tail], axis=0))
            v = pltpu.roll(m[0:16], 1, 1) + m[16:32] + pltpu.roll(m[32:48], L - 1, 1)
            v = leaky(v)
            bad = (lane == 1) & (gy == 0) | (lane == NYL + 2) & (gy == ngy - 1)
            if j == 0:
                bad = bad | (gx == 0)
            if j == HX - 1:
                bad = bad | (gx == ngx - 1)
            hn[j] = jnp.where(bad, 0.0, v).astype(BF)

    def boxes(lay, fields, pairs, xqs):
        acc = None
        for k in range(5):
            cols = []
            for x0, y0 in pairs:
                rows = []
                for p in range(16 * k, min(16 * k + 16, 72)):
                    g, yr = divmod(p, 6)
                    rows.append(fields[g // 4][x0 + g % 4, y0 + yr])
                if k == 4:
                    rows.append(ones[...])
                cols.append(jnp.concatenate(rows, axis=0))
            t = dots(tm[lay, 64 * xqs[0]:64 * xqs[-1] + 64, 256 * k:256 * k + 256], jnp.concatenate(cols, axis=1))
            acc = t if acc is None else acc + t
        return leaky(acc).astype(BF)

    def layer(lay, fields, todo, xqs, put):
        for h in range(0, len(todo), 2):
            pairs = todo[h:h + 2]
            v = boxes(lay, fields, pairs, xqs)
            for k, (x0, y0) in enumerate(pairs):
                b = v[:, L * k:L * k + L].reshape(len(xqs), 4, C, L)
                for i, xq in enumerate(xqs):
                    for yq in range(4):
                        put(x0 + xq, y0 + yq, b[i, yq])

    def layer_a(sec, f, todo, xqs=(0, 1)):
        xs = sorted({x0 + xq for x0, _ in todo for xq in xqs})
        ns = {x: pltpu.roll(hn[x], edge, 1) for x in xs}
        def put(x, y, t):
            h0[x, y] = t
            hm[x, y], hp[x, y] = shifted(t, ns[x], y + 1)
        layer(2 * sec, (fm, f, fp), todo, xqs, put)

    def outside():
        for r in (h0, hm, hp):
            pl.when(gx == 0)(lambda r=r: clear(r, 0, 1, 0, HY))
            pl.when(gx == ngx - 1)(lambda r=r: clear(r, HX - 1, HX, 0, HY))
            pl.when(gy == 0)(lambda r=r: clear(r, 0, HX, 0, 1))
            pl.when(gy == ngy - 1)(lambda r=r: clear(r, 0, HX, NYL + 1, NYL + 2))

    def layer_b(sec, g, o, todo, xqs=(0, 1)):
        def put(x, y, t):
            g[o + x, o + y] = t
        layer(2 * sec + 1, (hm, h0, hp), todo, xqs, put)

    def send_out(q, g, o, x, y):
        ab = [g[o + x + k, pl.ds(o + y, 16)].reshape(256, L) for k in range(2)]
        t = dots(pm[...], jnp.concatenate(ab, axis=1)).astype(BF)
        for k in range(2):
            stage[q, :, x + k, y:y + 16, :] = t[:, L * k:L * k + L].reshape(C, 16, L)
        pl.when(seg == q)(lambda: lcopy(q, x, y).start())
        pl.when(seg != q)(lambda: ocopy(q, x, y).start())

    def boxes_of(xs, ny, first=0):
        return [(x, y) for y in range(first, ny, 4) for x in xs]

    near, far = (0, 3), (1, 2)
    start_faces(0, f1, eb1, 0)
    start_sides(0, f1, eb1, yb1, (0, 1, 2, 3))
    wl.wait()
    bl.wait()
    wcopy(0, wall).start()
    wcopy(1, ball).start()
    pass_on(0, f1, eb1, yb1, near, 0)
    start_faces(0, f1, eb1, 1)
    pass_on(0, f1, eb1, yb1, far, 1)
    brow[...] = jnp.zeros_like(brow)
    wcopy(0, wall, 1 - seg).wait_recv()
    wcopy(1, ball, 1 - seg).wait_recv()
    wcopy(0, wall).wait_send()
    wcopy(1, ball).wait_send()
    for f in (f1, f2, fm, fp):
        clear(f, 0, FX, NYL + 4, FY)
    for sec in range(2):
        make_weights(sec)

    arrive(0, f1, eb1, 0)
    shift(f1, eb1, range(1, FX - 1))
    strips(0, eb1, range(1, HX - 1))
    layer_a(0, f1, boxes_of((1, 3), HY))
    outside()
    layer_b(0, f2, 2, boxes_of((1,), NYL))
    start_faces(1, f2, eb2, 1)
    start_sides(1, f2, eb2, yb2, far)
    for part, (y0, y1, y2) in enumerate(((0, HY, NYL),)):
        arrive(0, f1, eb1, 1, range(5))
        shift(f1, eb1, (0, FX - 1), 0, NYL + 4)
        if part == 0:
            strips(0, eb1, (0, HX - 1))
        layer_a(0, f1, boxes_of((0,), y1, y0), (0,))
        layer_a(0, f1, boxes_of((4,), y1, y0), (1,))
        outside()
        layer_b(0, f2, 2, boxes_of((0,), y2, 16 * part), (0,))
        layer_b(0, f2, 2, boxes_of((2,), y2, 16 * part), (1,))
        start_faces(1, f2, eb2, 0, (0, 4))

    start_sides(1, f2, eb2, yb2, near)
    for y in (0, 16):
        for x in (0, 2):
            send_out(0, f2, 2, x, y)
    pass_on(1, f2, eb2, yb2, far, 1)
    pass_on(1, f2, eb2, yb2, near, 0)
    shift(f2, eb2, range(2, FX - 2))
    strips(1, eb2, (2, 3))
    layer_a(1, f2, boxes_of((2,), HY))
    arrive(1, f2, eb2, 1)
    shift(f2, eb2, (0, FX - 1))
    arrive(1, f2, eb2, 0)
    shift(f2, eb2, (1, FX - 2))
    strips(1, eb2, (0, 1, 4, 5))
    layer_a(1, f2, boxes_of((0, 4), HY))
    outside()
    for y in (0, 16):
        for x in (0, 2):
            layer_b(1, res, 0, boxes_of((x,), y + 16, y))
    for y in (0, 16):
        for x in (0, 2):
            send_out(1, res, 0, x, y)
    drain(0, f1, eb1)
    drain(1, f2, eb2)

    for q in range(2):
        for y in (0, 16):
            for x in (0, 2):
                @pl.when(seg == q)
                def _(q=q, x=x, y=y):
                    lcopy(q, x, y).wait()
                    ocopy(q, x, y, 1 - seg).wait_recv()
                @pl.when(seg != q)
                def _(q=q, x=x, y=y):
                    ocopy(q, x, y).wait_send()


def shards(sizes, features, weights, biases):
    w = weights[0].transpose(0, 3, 4, 5, 1, 2).reshape(2, 27, C, C)
    hbm = pl.BlockSpec(memory_space=pltpu.HBM)
    dma = pltpu.SemaphoreType.DMA
    out = pl.pallas_call(
        functools.partial(kernel, sizes),
        name="sections",
        out_shape=jax.ShapeDtypeStruct((2, C, NXL, NYL, L), BF),
        in_specs=[hbm] * 3,
        out_specs=pl.BlockSpec(memory_space=pltpu.VMEM),
        scratch_shapes=[
            pltpu.VMEM((C, NXL, NYL, L), BF),
            pltpu.VMEM((2, 2, 27, C, C), BF),
            pltpu.VMEM((2, 2, C), BF),
            pltpu.VMEM((FX, FY, C, L), BF),
            pltpu.VMEM((FX, FY, C, L), BF),
            pltpu.VMEM((FX, FY, C, L), BF),
            pltpu.VMEM((FX, FY, C, L), BF),
            pltpu.VMEM((HX, HY, C, L), BF),
            pltpu.VMEM((HX, HY, C, L), BF),
            pltpu.VMEM((HX, HY, C, L), BF),
            pltpu.VMEM((4, L, KT), BF),
            pltpu.VMEM((2, 48, 256), BF),
            pltpu.VMEM((3, C, 384), F32),
            pltpu.VMEM((8, L), F32),
            pltpu.VMEM((48, 256), F32),
            pltpu.VMEM((256, 256), BF),
            pltpu.VMEM((L, L), BF),
            pltpu.VMEM((NYL * L, L), BF),
            pltpu.VMEM((2, FX, C, L), BF),
            pltpu.VMEM((2, FX, C, L), BF),
            pltpu.VMEM((2, 2, NXL, C, L), BF),
            pltpu.VMEM((2, 2, NXL, C, L), BF),
            pltpu.VMEM((HX, C, L), BF),
            pltpu.VMEM((NXL, NYL, C, L), BF),
            pltpu.VMEM((2, C, NXL, NYL, L), BF),
            dma((3,)), dma((2,)), dma((2,)),
            dma((2, 2, 2, 5)), dma((2, 2, 2, 5)),
            dma((2, 2, NXL)), dma((2, 2, NXL)),
            dma((2, 2, 2, NXL)), dma((2, 2, 2, NXL)),
            dma((2, NXL)), dma((2, NXL)), dma((2, 4)), dma((2, 4)), dma((2, 4)),
        ],
        compiler_params=pltpu.CompilerParams(
            collective_id=0, has_side_effects=True, vmem_limit_bytes=32 << 20),
    )(*(pltpu.with_memory_space_constraint(a, pltpu.HBM) for a in (features, w, biases[0])))
    return out[None]


def solution(mesh):
    placed = (
        P(None, None, "gx", "gy", "gz"),
        P("segment", None, None, None, None, None, None),
        P("segment", None, None),
    )
    sizes = (mesh.shape["gx"], mesh.shape["gy"])
    return jax.shard_map(
        functools.partial(shards, sizes),
        mesh=mesh,
        in_specs=placed,
        out_specs=P("segment", None, None, "gx", "gy", "gz"),
        check_vma=False,
    )
```
